32 devices in a mesh: row: 4 (over x, core), col: 8 (over z, y).
Axes of the slice: x: 2, y: 2, z: 4, core: 2. Of those that a mesh axis runs over, the one named last changes fastest.
Arguments:
- inputs: bfloat16 [512, 6144], P('col', 'row'), may hold values from -6 to 6
- cotangent: bfloat16 [512, 6144], P('col', 'row'), may hold values from -6 to 6
- weight_in: bfloat16 [6144, 12288], P('row', 'col'), may hold values from -0.078125 to 0.078125
- moment_in: bfloat16 [6144, 12288], P('row', 'col'), may hold values from -5 to 5
- second_in: bfloat16 [6144, 12288], P('row', 'col'), may hold values from 0.049804688 to 2
- weight_out: bfloat16 [12288, 6144], P('col', 'row'), may hold values from -0.0546875 to 0.0546875
- moment_out: bfloat16 [12288, 6144], P('col', 'row'), may hold values from -5 to 5
- second_out: bfloat16 [12288, 6144], P('col', 'row'), may hold values from 0.049804688 to 2
Outputs:
- input_grad: bfloat16 [512, 6144], P('col', 'row')
- update_in: bfloat16 [6144, 12288], P('row', 'col')
- code_moment_in: bfloat16 [6144, 12288], P('row', 'col')
- code_second_in: bfloat16 [6144, 12288], P('row', 'col')
- row_scale_in: float32 [2, 6144], P(None, 'row')
- col_scale_in: float32 [2, 12288], P(None, 'col')
- update_out: bfloat16 [12288, 6144], P('col', 'row')
- code_moment_out: bfloat16 [12288, 6144], P('col', 'row')
- code_second_out: bfloat16 [12288, 6144], P('col', 'row')
- row_scale_out: float32 [2, 12288], P(None, 'col')
- col_scale_out: float32 [2, 6144], P(None, 'row')
The draws below stay inside these ranges and needn't reach their ends.
All inputs are finite; a program needn't handle non-finite values. Where the reference program divides by a largest or mean magnitude, that divisor is 1e-20 or more.
Results may differ from the reference program's by a relative error of at most 0.0049.
Values may be sent and summed in bfloat16 or wider, within the bound.
A program may use at most 192 MiB of HBM per device.

```python
import math
import jax
import jax.numpy as jnp
from jax import lax

D = 6144
FF = 12288
TOKENS = 512


def block_levels(rng, shape, pieces, least, largest):
    loudness, own = 1.0, jax.random.fold_in(rng, 6)
    for axis_at, parts in pieces:
        steps = jnp.exp(jax.random.uniform(jax.random.fold_in(own, axis_at), (parts,), jnp.float32, least / len(pieces), largest / len(pieces)))
        loudness = loudness * jnp.repeat(steps, shape[axis_at] // parts).reshape([-1 if axis == axis_at else 1 for axis in range(len(shape))])
    return loudness


def noise(key, shape, spread, most, split=(), kind=jnp.bfloat16):
    array = spread * jax.random.normal(key, shape, jnp.float32)
    if split:
        array = array * block_levels(key, shape, split, -0.22, 0.18)
    return jnp.clip(array, -most, most).astype(kind)


def setup_inputs(seed: int = 0) -> dict:
    keys = jax.random.split(jax.random.key(seed), 9)
    return {
        "inputs": noise(keys[0], (TOKENS, D), 1.0, 6.0, ((0, 8), (1, 4))),
        "cotangent": noise(keys[1], (TOKENS, D), 1.0, 6.0, ((0, 8), (1, 4))),
        "weight_in": noise(keys[2], (D, FF), D ** -0.5, 0.078125, ((0, 4), (1, 8))),
        "moment_in": noise(keys[3], (D, FF), 1.0, 5.0, ((0, 4), (1, 8))),
        "second_in": jnp.clip(jnp.exp(math.log(2.0) - 3.6927934 * jax.random.uniform(keys[4], (D, FF), jnp.float32) ** block_levels(keys[4], (D, FF), ((0, 4), (1, 8)), -0.2, 0.2)), 0.049804688, 2.0).astype(jnp.bfloat16),
        "weight_out": noise(keys[5], (FF, D), FF ** -0.5, 0.0546875, ((0, 8), (1, 4))),
        "moment_out": noise(keys[6], (FF, D), 1.0, 5.0, ((0, 8), (1, 4))),
        "second_out": jnp.clip(jnp.exp(math.log(2.0) - 3.6927934 * jax.random.uniform(keys[7], (FF, D), jnp.float32) ** block_levels(keys[7], (FF, D), ((0, 8), (1, 4)), -0.2, 0.2)), 0.049804688, 2.0).astype(jnp.bfloat16),
    }


root_half = 0.7071067811865476
normal_density = 0.3989422804014327
momentum_decay = 0.9
second_decay = 0.95
stable_eps = 1e-08
weight_decay = 0.1

def gelu_parts(preact):
    cumulative = 0.5 * (1.0 + lax.erf(preact * root_half))
    density = jnp.exp(-0.5 * preact * preact) * normal_density
    return (preact * cumulative, cumulative + preact * density)

def optimize(weight, moment, second, gradient, factor):
    scaled = gradient * factor
    moment_new = momentum_decay * moment.astype(jnp.float32) + (1.0 - momentum_decay) * scaled
    second_new = second_decay * second.astype(jnp.float32) + (1.0 - second_decay) * scaled * scaled
    update = moment_new / (jnp.sqrt(second_new) + stable_eps) + weight_decay * weight.astype(jnp.float32)
    row_top = jnp.maximum(jnp.stack([lax.optimization_barrier(jnp.max(jnp.abs(moment_new), axis=1)), lax.optimization_barrier(jnp.max(second_new, axis=1))]), 1.0)
    col_top = jnp.maximum(jnp.stack([lax.optimization_barrier(jnp.max(jnp.abs(moment_new), axis=0)), lax.optimization_barrier(jnp.max(second_new, axis=0))]), 1.0)
    code_moment = moment_new / jnp.minimum(row_top[0][:, None], col_top[0][None, :])
    code_second = second_new / jnp.minimum(row_top[1][:, None], col_top[1][None, :])
    return (update.astype(jnp.bfloat16), code_moment.astype(jnp.bfloat16), code_second.astype(jnp.bfloat16), row_top, col_top)

def reference(inputs, cotangent, weight_in, moment_in, second_in, weight_out, moment_out, second_out):
    preact = jnp.dot(inputs, weight_in, preferred_element_type=jnp.float32)
    hidden_grad = jnp.dot(cotangent, weight_out.T, preferred_element_type=jnp.float32)
    activ_value, slope = gelu_parts(preact)
    hidden = activ_value.astype(jnp.bfloat16)
    delta = (hidden_grad * slope).astype(jnp.bfloat16)
    input_grad = jnp.dot(delta, weight_in.T, preferred_element_type=jnp.float32).astype(jnp.bfloat16)
    grad_in = jnp.dot(inputs.T, delta, preferred_element_type=jnp.float32)
    grad_out = jnp.dot(hidden.T, cotangent, preferred_element_type=jnp.float32)
    total = jnp.sum(grad_in * grad_in) + jnp.sum(grad_out * grad_out)
    factor = 1.0 / jnp.maximum(jnp.sqrt(total / (2.0 * D * FF)), 1.0)
    first = optimize(weight_in, moment_in, second_in, grad_in, factor)
    latter = optimize(weight_out, moment_out, second_out, grad_out, factor)
    return (input_grad, first[0], first[1], first[2], first[3], first[4], latter[0], latter[1], latter[2], latter[3], latter[4])
```

```python
import functools

import jax
import jax.numpy as jnp
from jax import lax
from jax.experimental import pallas as pl
from jax.experimental.pallas import tpu as pltpu
from jax.sharding import PartitionSpec as P

root_half = 0.7071067811865476
normal_density = 0.3989422804014327
momentum_decay = 0.9
second_decay = 0.95
stable_eps = 1e-08
weight_decay = 0.1
LANES = 128


def contract(left, right, left_dim, right_dim):
    return lax.dot_general(
        left, right, (((left_dim,), (right_dim,)), ((), ())), preferred_element_type=jnp.float32
    )


def activate(preact, hidden_grad):
    cumulative = 0.5 * (1.0 + lax.erf(preact * root_half))
    density = jnp.exp(-0.5 * preact * preact) * normal_density
    hidden = (preact * cumulative).astype(jnp.bfloat16)
    delta = (hidden_grad * (cumulative + preact * density)).astype(jnp.bfloat16)
    return (hidden, delta)


MESH = pl.DeviceIdType.MESH


def remote(source, target, send, receive, axis, peer):
    return pltpu.make_async_remote_copy(
        src_ref=source,
        dst_ref=target,
        send_sem=send,
        recv_sem=receive,
        device_id={axis: peer},
        device_id_type=MESH,
    )


def span(start, size):
    return pl.ds(pl.multiple_of(start, size), size)


def lane_tile(size):
    return 512 if size % 512 == 0 else 256 if size % 256 == 0 else 128


def folded(values):
    total = values[:8, :LANES] * 0.0
    for low in range(0, values.shape[0], 8):
        for at in range(0, values.shape[1], LANES):
            total = total + values[low : low + 8, at : at + LANES]
    return total


def front_kernel(
    shape, x_ref, c_ref, wi_hbm, wo_hbm,
    x_out, c_out, hidden_out, delta_out, grad_ref, factor_ref,
    acts, wi, wo, pair_send, pair_recv, pair_own, line_send, line_recv, line_own, hd,
    dx_own, dx_send, dx_recv, dz_send, dz_recv, part_ref, col_tops, row_tops, grams,
    load_sem, z_send, z_recv, y_send, y_recv, pair_s, pair_r, line_s, line_r,
    gather_s, gather_r, share_s, share_r, dy_s, dy_r, dz_s, dz_r,
    tot_s, tot_r, row_s, row_r, out_sem,
):
    rows, cols, nx, ny, nz, entries = shape
    t, width = x_ref.shape
    hidden = wi.shape[1]
    size = ny * t
    half = size // 2
    piece = half // nx
    tokens = size * nz
    r, k = lax.axis_index("row"), lax.axis_index("col")
    x, core = r // 2, r % 2
    z, y = k // ny, k % ny
    partner = x * 2 + (1 - core)
    below, above = z, nz - 1 - z
    middle = jnp.minimum(below, above)

    def source_of(g):
        if g == 0:
            return z, 0
        near = g <= 2 * middle
        distance = jnp.where(near, (g + 1) // 2, g - middle)
        side = jnp.where(near, -1 if g % 2 else 1, jnp.where(above > below, 1, -1))
        return z + side * distance, side

    order = [source_of(g) for g in range(nz)]

    def line_peer(off):
        return lax.rem(x + off, nx) * 2 + core

    def y_peer(off):
        return z * ny + lax.rem(y + off, ny)

    loads = [
        pltpu.make_async_copy(x_ref, acts.at[0, span(k * t, t)], load_sem.at[0]),
        pltpu.make_async_copy(c_ref, acts.at[1, span(k * t, t)], load_sem.at[1]),
        pltpu.make_async_copy(wi_hbm, wi, load_sem.at[2]),
        pltpu.make_async_copy(wo_hbm, wo, load_sem.at[3]),
    ]
    for load in loads:
        load.start()
    barrier = pltpu.get_barrier_semaphore()
    for off in range(1, cols):
        pl.semaphore_signal(
            barrier, inc=1, device_id={"col": lax.rem(k + off, cols)}, device_id_type=MESH
        )
    for off in range(1, rows):
        pl.semaphore_signal(
            barrier, inc=1, device_id={"row": lax.rem(r + off, rows)}, device_id_type=MESH
        )
    loads[0].wait()
    loads[1].wait()
    pl.semaphore_wait(barrier, cols + rows - 2)

    pending = []

    def z_copy(item, zs, g, way, sign):
        block = acts.at[item, span((zs * ny + y) * t, t)]
        return remote(
            block, block, z_send.at[item, g, way], z_recv.at[item, zs], "col", (z + sign) * ny + y
        )

    def y_copies(item, zs, g):
        block = acts.at[item, span((zs * ny + y) * t, t)]
        copies = [
            remote(
                block, block, y_send.at[item, g, off], y_recv.at[item, zs, y], "col", y_peer(off)
            )
            for off in range(1, ny)
        ]
        for copy in copies:
            copy.start()
            pending.append(copy)

    ways = ((0, 1, z < nz - 1), (1, -1, z > 0))
    for item in range(2):
        for way, sign, there in ways:
            pl.when(there)(lambda i=item, w=way, s=sign: z_copy(i, z, 0, w, s).start())
        y_copies(item, z, 0)

    def onward(g):
        zs, side = order[g]
        ahead = z - side
        return zs, -side, jnp.logical_and(ahead >= 0, ahead < nz)

    def forward(g):
        zs, sign, there = onward(g)
        for item in range(2):
            block = acts.at[item, span((zs * ny + y) * t, t)]
            remote(
                block, block, z_send.at[item, g, 0], z_recv.at[item, zs], "col", y_peer(1)
            ).wait_recv()
            pl.when(there)(lambda i=item: z_copy(i, zs, g, 0, sign).start())
            y_copies(item, zs, g)

    def y_wait(g, item):
        zs, _ = order[g]
        for off in range(1, ny):
            ys = lax.rem(y + off, ny)
            block = acts.at[item, span((zs * ny + ys) * t, t)]
            remote(
                block, block, y_send.at[item, g, off], y_recv.at[item, zs, ys], "col", y_peer(1)
            ).wait_recv()

    tile_h, tile_w = lane_tile(hidden), lane_tile(width)

    def forward_product(g, item):
        first = order[g][0] * size
        left = jnp.concatenate(
            [
                acts[item, span(first + (1 - core) * half, half), :],
                acts[item, span(first + core * half, half), :],
            ],
            axis=0,
        )

        @pl.loop(0, hidden // tile_h)
        def _(n):
            at = span(n * tile_h, tile_h)
            if item == 0:
                part = contract(left, wi[:, at], 1, 0)
            else:
                part = contract(left, wo[at, :], 1, 1)
            pair_send[g, item, :, at] = part[:half]
            pair_own[g, item, :, at] = part[half:]

        pair_copy(g, item).start()
        pending.append(pair_copy(g, item))

    def pair_copy(g, item):
        return remote(
            pair_send.at[g, item], pair_recv.at[g, item],
            pair_s.at[g, item], pair_r.at[g, item], "row", partner,
        )

    def line_copy(g, off):
        return remote(
            line_send.at[g, off - 1], line_recv.at[g, off - 1],
            line_s.at[g, off], line_r.at[g, off], "row", line_peer(off),
        )

    def pair_sum(g):
        for item in range(2):
            pair_copy(g, item).wait_recv()
        for off in range(1, nx):
            take = span(lax.rem(x + off, nx) * piece, piece)
            for item in range(2):
                line_send[g, off - 1, item] = (
                    pair_own[g, item, take, :] + pair_recv[g, item, take, :]
                ).astype(jnp.bfloat16)
            line_copy(g, off).start()
            pending.append(line_copy(g, off))
        take = span(x * piece, piece)
        for item in range(2):
            line_own[g, item] = pair_own[g, item, take, :] + pair_recv[g, item, take, :]

    def gather_block(g, xs):
        return hd.at[:, span(order[g][0] * size + core * half + xs * piece, piece), :]

    def gather_copy(g, off):
        block = gather_block(g, x)
        return remote(
            block, block, gather_s.at[g, off], gather_r.at[g, off], "row", line_peer(off)
        )

    def active(g):
        for off in range(1, nx):
            line_copy(g, off).wait_recv()
        first = order[g][0] * size + core * half + x * piece

        @pl.loop(0, hidden // LANES)
        def _(n):
            at = span(n * LANES, LANES)
            preact, hidden_grad = line_own[g, 0, :, at], line_own[g, 1, :, at]
            for off in range(1, nx):
                preact = preact + line_recv[g, off - 1, 0, :, at].astype(jnp.float32)
                hidden_grad = hidden_grad + line_recv[g, off - 1, 1, :, at].astype(jnp.float32)
            value, slope = activate(preact, hidden_grad)
            hd[0, span(first, piece), at] = value
            hd[1, span(first, piece), at] = slope

        for off in range(1, nx):
            gather_copy(g, off).start()
            pending.append(gather_copy(g, off))

    def share_copy(g, which):
        block = hd.at[:, span(order[g][0] * size + which * half, half), :]
        return remote(block, block, share_s.at[g], share_r.at[g], "row", partner)

    def share(g):
        for off in range(1, nx):
            xs = lax.rem(x + nx - off, nx)
            block = gather_block(g, xs)
            remote(
                block, block, gather_s.at[g, off], gather_r.at[g, off], "row", line_peer(off)
            ).wait_recv()
        share_copy(g, core).start()
        pending.append(share_copy(g, core))

    def share_wait(g):
        share_copy(g, 1 - core).wait_recv()

    def dx_copy(g, off):
        return remote(
            dx_send.at[g, off - 1], dx_recv.at[g, off - 1],
            dy_s.at[g, off], dy_r.at[g, off], "col", y_peer(off),
        )

    def back_product(groups):
        left = jnp.concatenate(
            [
                hd[1, span(order[g][0] * size + lax.rem(y + off, ny) * t, t), :]
                for g in groups
                for off in range(ny)
            ],
            axis=0,
        )

        @pl.loop(0, width // tile_w)
        def _(n):
            at = span(n * tile_w, tile_w)
            part = contract(left, wi[at, :], 1, 1)
            for i, g in enumerate(groups):
                for off in range(ny):
                    low = (i * ny + off) * t
                    if off == 0:
                        dx_own[g, :, at] = part[low : low + t]
                    else:
                        dx_send[g, off - 1, :, at] = part[low : low + t].astype(jnp.bfloat16)

        for g in groups:
            for off in range(1, ny):
                dx_copy(g, off).start()
                pending.append(dx_copy(g, off))

    def dz_copy(g):
        return remote(
            dz_send.at[g], dz_recv.at[z], dz_s.at[g], dz_r.at[z], "col", order[g][0] * ny + y
        )

    def back_sum(g):
        for off in range(1, ny):
            dx_copy(g, off).wait_recv()
        total = dx_own[g]
        for off in range(1, ny):
            total = total + dx_recv[g, off - 1].astype(jnp.float32)
        if g == 0:
            dx_own[0] = total
        else:
            dz_send[g] = total.astype(jnp.bfloat16)
            dz_copy(g).start()
            pending.append(dz_copy(g))

    outs = []

    def put(source, target, slot):
        copy = pltpu.make_async_copy(source, target, out_sem.at[slot])
        copy.start()
        outs.append(copy)

    use_grams = grams is not None
    tile_t = 256 if tokens % 256 == 0 else 128

    def gram(which, source, item):
        @pl.loop(0, tokens // tile_t)
        def _(n):
            at = span(n * tile_t, tile_t)
            grams[which, :, at] = contract(source[item], source[item, at, :], 1, 1)

    def local_total():
        if use_grams:
            part_ref[...] = jnp.zeros_like(part_ref)

            @pl.loop(0, tokens // tile_t)
            def _(n):
                at = span(n * tile_t, tile_t)
                late_in = contract(hd[1], hd[1, at, :], 1, 1)
                part_ref[...] += folded(late_in * grams[0, :, at])
                late_out = contract(hd[0], hd[0, at, :], 1, 1)
                part_ref[...] += folded(late_out * grams[1, :, at])
        else:
            part_ref[...] = jnp.zeros_like(part_ref)
            for left, right, count in ((acts.at[0], hd.at[1], width), (hd.at[0], acts.at[1], hidden)):

                @pl.loop(0, count // LANES)
                def _(n):
                    at = span(n * LANES, LANES)
                    part = contract(left[:, at], right[...], 0, 0)
                    part_ref[...] += folded(part * part)

    for s in range(nz + 3):
        if s + 1 < nz:
            forward(s + 1)
        if s < nz:
            for item in range(2):
                y_wait(s, item)
                if s == 0:
                    loads[2 + item].wait()
                forward_product(s, item)
        if 0 <= s - 1 < nz:
            active(s - 1)
        if s == nz - 1:
            put(acts.at[0], x_out, 0)
            put(acts.at[1], c_out, 1)
        if s < nz:
            pair_sum(s)
        if s == nz and use_grams:
            gram(0, acts, 0)
            gram(1, acts, 1)
        if 0 <= s - 2 < nz:
            share(s - 2)
        if 0 <= s - 3 < nz:
            share_wait(s - 3)
        if s == nz - 1:
            back_product(list(range(nz - 3)))
        if s == nz:
            back_product([nz - 3])
            for g in range(nz - 3):
                back_sum(g)
        if s == nz + 1:
            back_product([nz - 2])
            back_sum(nz - 3)
    put(hd.at[0], hidden_out, 2)
    put(hd.at[1], delta_out, 3)
    back_product([nz - 1])
    local_total()

    def col_copy(off):
        return remote(
            part_ref, col_tops.at[off], tot_s.at[off], tot_r.at[off],
            "col", lax.rem(k + off, cols),
        )

    def row_copy(off):
        return remote(
            col_tops.at[0], row_tops.at[off], row_s.at[off], row_r.at[off],
            "row", lax.rem(r + off, rows),
        )

    for off in range(1, cols):
        col_copy(off).start()
        pending.append(col_copy(off))
    back_sum(nz - 2)
    back_sum(nz - 1)
    for off in range(1, cols):
        col_copy(off).wait_recv()
    total = part_ref[...]
    for off in range(1, cols):
        total = total + col_tops[off]
    col_tops[0] = total
    for off in range(1, rows):
        row_copy(off).start()
        pending.append(row_copy(off))
    for off in range(1, rows):
        row_copy(off).wait_recv()
        total = total + row_tops[off]
    total = jnp.sum(jnp.sum(total, axis=0, keepdims=True), axis=1, keepdims=True)
    total = jnp.maximum(total, 0.0)
    factor = 1.0 / jnp.maximum(jnp.sqrt(total / entries), 1.0)
    factor_ref[...] = jnp.broadcast_to(factor, factor_ref.shape)

    total = dx_own[0]
    for off in range(1, nz):
        zs = lax.rem(z + off, nz)
        remote(
            dz_send.at[1], dz_recv.at[zs], dz_s.at[1], dz_r.at[zs], "col", y_peer(1)
        ).wait_recv()
        total = total + dz_recv[zs].astype(jnp.float32)
    grad_ref[...] = total.astype(jnp.bfloat16)

    for item in range(2):
        for way, sign, there in ways:
            pl.when(there)(lambda i=item, w=way, s=sign: z_copy(i, z, 0, w, s).wait_send())
    for g in range(1, nz):
        zs, sign, there = onward(g)
        for item in range(2):
            pl.when(there)(lambda i=item, a=zs, b=g, s=sign: z_copy(i, a, b, 0, s).wait_send())
    for copy in pending:
        copy.wait_send()
    for copy in outs:
        copy.wait()


def front(sizes, inputs, cotangent, weight_in, weight_out):
    rows, cols = sizes["row"], sizes["col"]
    nx = rows // 2
    ny = 2 ** ((cols.bit_length() - 1) // 2)
    nz = cols // ny
    t, width = inputs.shape
    hidden = weight_in.shape[1]
    size = t * ny
    half, tokens = size // 2, size * nz
    piece = half // nx
    entries = 2.0 * width * rows * hidden * cols
    bf, f4 = jnp.bfloat16, jnp.float32
    use_grams = tokens <= hidden
    dma = lambda *dims: pltpu.SemaphoreType.DMA(dims)
    scratch = [
        pltpu.VMEM((2, tokens, width), bf),
        pltpu.VMEM(weight_in.shape, bf),
        pltpu.VMEM(weight_out.shape, bf),
        pltpu.VMEM((nz, 2, half, hidden), f4),
        pltpu.VMEM((nz, 2, half, hidden), f4),
        pltpu.VMEM((nz, 2, half, hidden), f4),
        pltpu.VMEM((nz, nx - 1, 2, piece, hidden), bf),
        pltpu.VMEM((nz, nx - 1, 2, piece, hidden), bf),
        pltpu.VMEM((nz, 2, piece, hidden), f4),
        pltpu.VMEM((2, tokens, hidden), bf),
        pltpu.VMEM((nz, t, width), f4),
        pltpu.VMEM((nz, ny - 1, t, width), bf),
        pltpu.VMEM((nz, ny - 1, t, width), bf),
        pltpu.VMEM((nz, t, width), bf),
        pltpu.VMEM((nz, t, width), bf),
        pltpu.VMEM((8, LANES), f4),
        pltpu.VMEM((cols, 8, LANES), f4),
        pltpu.VMEM((rows, 8, LANES), f4),
        pltpu.VMEM((2, tokens, tokens), f4) if use_grams else None,
        dma(4),
        dma(2, nz, 2), dma(2, nz), dma(2, nz, ny), dma(2, nz, ny),
        dma(nz, 2), dma(nz, 2), dma(nz, nx), dma(nz, nx),
        dma(nz, nx), dma(nz, nx), dma(nz), dma(nz),
        dma(nz, ny), dma(nz, ny), dma(nz), dma(nz),
        dma(cols), dma(cols), dma(rows), dma(rows), dma(4),
    ]
    kept = [item for item in scratch if item is not None]
    slot = 10 + scratch.index(None) if None in scratch else None

    def kernel(*refs):
        refs = list(refs)
        if slot is not None:
            refs.insert(slot, None)
        front_kernel((rows, cols, nx, ny, nz, entries), *refs)

    anywhere = pl.BlockSpec(memory_space=pl.ANY)
    inside = pl.BlockSpec(memory_space=pltpu.VMEM)
    return pl.pallas_call(
        kernel,
        out_shape=[
            jax.ShapeDtypeStruct((tokens, width), bf),
            jax.ShapeDtypeStruct((tokens, width), bf),
            jax.ShapeDtypeStruct((tokens, hidden), bf),
            jax.ShapeDtypeStruct((tokens, hidden), bf),
            jax.ShapeDtypeStruct((t, width), bf),
            jax.ShapeDtypeStruct((8, LANES), f4),
        ],
        in_specs=[anywhere] * 4,
        out_specs=[anywhere] * 4 + [inside] * 2,
        scratch_shapes=kept,
        compiler_params=pltpu.CompilerParams(
            collective_id=0, has_side_effects=True, vmem_limit_bytes=60 * 2**20
        ),
        name="front",
    )(inputs, cotangent, weight_in, weight_out)


def exchange_kernel(plan, sizes, *refs):
    count = len(plan)
    sources, targets = refs[:count], refs[count : 2 * count]
    send_sem, recv_sem, own_sem = refs[2 * count :]
    axes = sorted(set(axis for axis, _ in plan))
    me = {axis: lax.axis_index(axis) for axis in axes}
    barrier = pltpu.get_barrier_semaphore()
    greeted = 0
    for axis in axes:
        for step in range(1, sizes[axis]):
            peer = lax.rem(me[axis] + step, sizes[axis])
            pl.semaphore_signal(
                barrier, inc=1, device_id={axis: peer}, device_id_type=pl.DeviceIdType.MESH
            )
            greeted += 1
    owns = []
    for item, (axis, scatter) in enumerate(plan):
        block = sources[item].at[me[axis]] if scatter else sources[item]
        own = pltpu.make_async_copy(block, targets[item].at[me[axis]], own_sem.at[item])
        own.start()
        owns.append(own)
    pl.semaphore_wait(barrier, greeted)
    copies = []
    at = 0
    for item, (axis, scatter) in enumerate(plan):
        for step in range(1, sizes[axis]):
            peer = lax.rem(me[axis] + step, sizes[axis])
            block = sources[item].at[peer] if scatter else sources[item]
            copy = pltpu.make_async_remote_copy(
                src_ref=block,
                dst_ref=targets[item].at[me[axis]],
                send_sem=send_sem.at[at],
                recv_sem=recv_sem.at[at],
                device_id={axis: peer},
                device_id_type=pl.DeviceIdType.MESH,
            )
            copy.start()
            copies.append(copy)
            at += 1
    for own in owns:
        own.wait()
    for copy in copies:
        copy.wait()


def exchange(identity, plan, sizes, *arrays):
    flights = sum(sizes[axis] - 1 for axis, _ in plan)
    shapes = [
        jax.ShapeDtypeStruct(
            array.shape if scatter else (sizes[axis],) + array.shape, array.dtype
        )
        for array, (axis, scatter) in zip(arrays, plan)
    ]
    return pl.pallas_call(
        functools.partial(exchange_kernel, plan, sizes),
        out_shape=shapes,
        in_specs=[pl.BlockSpec(memory_space=pl.ANY)] * len(plan),
        out_specs=[pl.BlockSpec(memory_space=pl.ANY)] * len(plan),
        scratch_shapes=[
            pltpu.SemaphoreType.DMA((flights,)),
            pltpu.SemaphoreType.DMA((flights,)),
            pltpu.SemaphoreType.DMA((len(plan),)),
        ],
        compiler_params=pltpu.CompilerParams(collective_id=identity, has_side_effects=True),
        name=f"exchange{identity}",
    )(*arrays)


def lane_fold(values, combine):
    folded = values[:, :LANES]
    for at in range(LANES, values.shape[1], LANES):
        folded = combine(folded, values[:, at : at + LANES])
    return folded


def row_block(rows):
    return 256 if rows % 256 == 0 else 128


def to_lanes(column_tops):
    pieces = []
    for at in range(0, column_tops.shape[0], LANES):
        turned = column_tops[at : at + LANES].T
        pieces.append(jnp.max(turned, axis=0, keepdims=True))
    return jnp.concatenate(pieces, axis=1)


def moments_kernel(
    factor_ref, left_ref, right_ref, weight_ref, moment_ref, second_ref,
    update_ref, new_moment_ref, new_second_ref, row_ref, col_ref,
):
    gradient = contract(left_ref[...], right_ref[...], 0, 0)
    scaled = gradient * factor_ref[0:1, 0:1]
    moment_new = momentum_decay * moment_ref[...].astype(jnp.float32) + (
        1.0 - momentum_decay
    ) * scaled
    second_new = second_decay * second_ref[...].astype(jnp.float32) + (
        1.0 - second_decay
    ) * scaled * scaled
    update = moment_new / (jnp.sqrt(second_new) + stable_eps) + weight_decay * weight_ref[
        ...
    ].astype(jnp.float32)
    update_ref[...] = update.astype(jnp.bfloat16)
    new_moment_ref[...] = moment_new.astype(jnp.bfloat16)
    new_second_ref[...] = second_new.astype(jnp.bfloat16)
    size = jnp.abs(moment_new)
    row_ref[0:1, :] = to_lanes(lane_fold(size, jnp.maximum))
    row_ref[1:2, :] = to_lanes(lane_fold(second_new, jnp.maximum))

    @pl.when(pl.program_id(0) == 0)
    def _():
        col_ref[...] = jnp.zeros_like(col_ref)

    col_ref[0:1, :] = jnp.maximum(col_ref[0:1, :], jnp.max(size, axis=0, keepdims=True))
    col_ref[1:2, :] = jnp.maximum(col_ref[1:2, :], jnp.max(second_new, axis=0, keepdims=True))


def moments(factor, left, right, weight, moment, second):
    rows, cols = weight.shape
    tokens = left.shape[0]
    block = row_block(rows)
    tile = pl.BlockSpec((block, cols), lambda i: (i, 0))
    half = jax.ShapeDtypeStruct((rows, cols), jnp.bfloat16)
    return pl.pallas_call(
        moments_kernel,
        grid=(rows // block,),
        out_shape=[
            half,
            half,
            half,
            jax.ShapeDtypeStruct((2, rows), jnp.float32),
            jax.ShapeDtypeStruct((2, cols), jnp.float32),
        ],
        in_specs=[
            pl.BlockSpec((8, LANES), lambda i: (0, 0)),
            pl.BlockSpec((tokens, block), lambda i: (0, i)),
            pl.BlockSpec((tokens, cols), lambda i: (0, 0)),
            tile,
            tile,
            tile,
        ],
        out_specs=[
            tile,
            tile,
            tile,
            pl.BlockSpec((2, block), lambda i: (0, i)),
            pl.BlockSpec((2, cols), lambda i: (0, 0)),
        ],
        name="moments",
    )(factor, left, right, weight, moment, second)


def encode_kernel(moment_ref, second_ref, row_ref, col_ref, code_moment_ref, code_second_ref):
    rows, cols = moment_ref.shape
    for which, (source, target) in enumerate(
        ((moment_ref, code_moment_ref), (second_ref, code_second_ref))
    ):
        for low in range(0, rows, LANES):
            span = pl.ds(low, LANES)
            inverse = 1.0 / row_ref[which : which + 1, low : low + LANES]
            inverse = jnp.broadcast_to(inverse, (LANES, LANES)).T
            for at in range(0, cols, LANES):
                other = 1.0 / col_ref[which : which + 1, at : at + LANES]
                value = source[span, at : at + LANES].astype(jnp.float32)
                target[span, at : at + LANES] = (value * jnp.maximum(inverse, other)).astype(
                    jnp.bfloat16
                )


def encode(moment, second, row_top, col_top):
    rows, cols = moment.shape
    block = row_block(rows)
    tile = pl.BlockSpec((block, cols), lambda i: (i, 0))
    half = jax.ShapeDtypeStruct((rows, cols), jnp.bfloat16)
    return pl.pallas_call(
        encode_kernel,
        grid=(rows // block,),
        out_shape=[half, half],
        in_specs=[
            tile,
            tile,
            pl.BlockSpec((2, block), lambda i: (0, i)),
            pl.BlockSpec((2, cols), lambda i: (0, 0)),
        ],
        out_specs=[tile, tile],
        name="encode",
    )(moment, second, row_top, col_top)


def shards(
    sizes, inputs, cotangent, weight_in, moment_in, second_in, weight_out, moment_out, second_out
):
    all_inputs, all_cotangent, all_hidden, all_delta, input_grad, factor = front(
        sizes, inputs, cotangent, weight_in, weight_out
    )
    update_in, moment_new_in, second_new_in, rows_in, cols_in = moments(
        factor, all_inputs, all_delta, weight_in, moment_in, second_in
    )
    update_out, moment_new_out, second_new_out, rows_out, cols_out = moments(
        factor, all_hidden, all_cotangent, weight_out, moment_out, second_out
    )
    rows_in, cols_out, cols_in, rows_out = exchange(
        5,
        (("col", False), ("col", False), ("row", False), ("row", False)),
        sizes,
        rows_in,
        cols_out,
        cols_in,
        rows_out,
    )
    rows_in, cols_out, cols_in, rows_out = (
        jnp.maximum(jnp.max(tops, axis=0), 1.0) for tops in (rows_in, cols_out, cols_in, rows_out)
    )
    code_moment_in, code_second_in = encode(moment_new_in, second_new_in, rows_in, cols_in)
    code_moment_out, code_second_out = encode(moment_new_out, second_new_out, rows_out, cols_out)
    return (
        input_grad,
        update_in,
        code_moment_in,
        code_second_in,
        rows_in,
        cols_in,
        update_out,
        code_moment_out,
        code_second_out,
        rows_out,
        cols_out,
    )


def solution(mesh):
    in_specs = (
        P("col", "row"),
        P("col", "row"),
        P("row", "col"),
        P("row", "col"),
        P("row", "col"),
        P("col", "row"),
        P("col", "row"),
        P("col", "row"),
    )
    out_specs = (
        P("col", "row"),
        P("row", "col"),
        P("row", "col"),
        P("row", "col"),
        P(None, "row"),
        P(None, "col"),
        P("col", "row"),
        P("col", "row"),
        P("col", "row"),
        P(None, "col"),
        P(None, "row"),
    )
    sizes = {axis: mesh.shape[axis] for axis in ("row", "col")}
    return jax.shard_map(
        functools.partial(shards, sizes),
        mesh=mesh,
        in_specs=in_specs,
        out_specs=out_specs,
        check_vma=False,
    )
```

```python
import functools

import jax
import jax.numpy as jnp
from jax import lax
from jax.experimental import pallas as pl
from jax.experimental.pallas import tpu as pltpu
from jax.sharding import PartitionSpec as P

root_half = 0.7071067811865476
normal_density = 0.3989422804014327
momentum_decay = 0.9
second_decay = 0.95
stable_eps = 1e-08
weight_decay = 0.1
LANES = 128
PACKED = 16
AHEAD = 2
VMEM_MOMENTS = 40 * 2**20
VMEM_ENCODE = 40 * 2**20


def contract(left, right, left_dim, right_dim):
    return lax.dot_general(
        left, right, (((left_dim,), (right_dim,)), ((), ())), preferred_element_type=jnp.float32
    )


def activate(preact, hidden_grad):
    cumulative = 0.5 * (1.0 + lax.erf(preact * root_half))
    density = jnp.exp(-0.5 * preact * preact) * normal_density
    hidden = (preact * cumulative).astype(jnp.bfloat16)
    delta = (hidden_grad * (cumulative + preact * density)).astype(jnp.bfloat16)
    return (hidden, delta)


MESH = pl.DeviceIdType.MESH


def remote(source, target, send, receive, axis, peer):
    return pltpu.make_async_remote_copy(
        src_ref=source,
        dst_ref=target,
        send_sem=send,
        recv_sem=receive,
        device_id={axis: peer},
        device_id_type=MESH,
    )


def span(start, size):
    return pl.ds(pl.multiple_of(start, size), size)


def lane_tile(size):
    return 512 if size % 512 == 0 else 256 if size % 256 == 0 else 128


def folded(values):
    total = values[:8, :LANES] * 0.0
    for low in range(0, values.shape[0], 8):
        for at in range(0, values.shape[1], LANES):
            total = total + values[low : low + 8, at : at + LANES]
    return total


def front_kernel(
    shape, x_ref, c_ref, wi_hbm, wo_hbm,
    x_out, c_out, hidden_out, delta_out, grad_ref, factor_ref,
    acts, wi, wo, pair_send, pair_recv, pair_own, line_send, line_recv, line_own, hd,
    dx_own, dx_send, dx_recv, dz_send, dz_recv, part_ref, col_tops, row_tops, grams,
    load_sem, z_send, z_recv, y_send, y_recv, pair_s, pair_r, line_s, line_r,
    gather_s, gather_r, share_s, share_r, dy_s, dy_r, dz_s, dz_r,
    tot_s, tot_r, row_s, row_r, out_sem,
):
    rows, cols, nx, ny, nz, entries = shape
    t, width = x_ref.shape
    hidden = wi.shape[1]
    size = ny * t
    half = size // 2
    piece = half // nx
    tokens = size * nz
    r, k = lax.axis_index("row"), lax.axis_index("col")
    x, core = r // 2, r % 2
    z, y = k // ny, k % ny
    partner = x * 2 + (1 - core)
    below, above = z, nz - 1 - z
    middle = jnp.minimum(below, above)

    def source_of(g):
        if g == 0:
            return z, 0
        near = g <= 2 * middle
        distance = jnp.where(near, (g + 1) // 2, g - middle)
        side = jnp.where(near, -1 if g % 2 else 1, jnp.where(above > below, 1, -1))
        return z + side * distance, side

    order = [source_of(g) for g in range(nz)]

    def line_peer(off):
        return lax.rem(x + off, nx) * 2 + core

    def y_peer(off):
        return z * ny + lax.rem(y + off, ny)

    loads = [
        pltpu.make_async_copy(x_ref, acts.at[0, span(k * t, t)], load_sem.at[0]),
        pltpu.make_async_copy(c_ref, acts.at[1, span(k * t, t)], load_sem.at[1]),
        pltpu.make_async_copy(wi_hbm, wi, load_sem.at[2]),
        pltpu.make_async_copy(wo_hbm, wo, load_sem.at[3]),
    ]
    for load in loads:
        load.start()
    barrier = pltpu.get_barrier_semaphore()
    for off in range(1, cols):
        pl.semaphore_signal(
            barrier, inc=1, device_id={"col": lax.rem(k + off, cols)}, device_id_type=MESH
        )
    for off in range(1, rows):
        pl.semaphore_signal(
            barrier, inc=1, device_id={"row": lax.rem(r + off, rows)}, device_id_type=MESH
        )
    loads[0].wait()
    loads[1].wait()
    pl.semaphore_wait(barrier, cols + rows - 2)

    pending = []

    def z_copy(item, zs, g, way, sign):
        block = acts.at[item, span((zs * ny + y) * t, t)]
        return remote(
            block, block, z_send.at[item, g, way], z_recv.at[item, zs], "col", (z + sign) * ny + y
        )

    def y_copies(item, zs, g):
        block = acts.at[item, span((zs * ny + y) * t, t)]
        copies = [
            remote(
                block, block, y_send.at[item, g, off], y_recv.at[item, zs, y], "col", y_peer(off)
            )
            for off in range(1, ny)
        ]
        for copy in copies:
            copy.start()
            pending.append(copy)

    ways = ((0, 1, z < nz - 1), (1, -1, z > 0))
    for item in range(2):
        for way, sign, there in ways:
            pl.when(there)(lambda i=item, w=way, s=sign: z_copy(i, z, 0, w, s).start())
        y_copies(item, z, 0)

    def onward(g):
        zs, side = order[g]
        ahead = z - side
        return zs, -side, jnp.logical_and(ahead >= 0, ahead < nz)

    def forward(g):
        zs, sign, there = onward(g)
        for item in range(2):
            block = acts.at[item, span((zs * ny + y) * t, t)]
            remote(
                block, block, z_send.at[item, g, 0], z_recv.at[item, zs], "col", y_peer(1)
            ).wait_recv()
            pl.when(there)(lambda i=item: z_copy(i, zs, g, 0, sign).start())
            y_copies(item, zs, g)

    def y_wait(g, item):
        zs, _ = order[g]
        for off in range(1, ny):
            ys = lax.rem(y + off, ny)
            block = acts.at[item, span((zs * ny + ys) * t, t)]
            remote(
                block, block, y_send.at[item, g, off], y_recv.at[item, zs, ys], "col", y_peer(1)
            ).wait_recv()

    tile_h, tile_w = lane_tile(hidden), lane_tile(width)

    def forward_product(g, item):
        first = order[g][0] * size
        left = jnp.concatenate(
            [
                acts[item, span(first + (1 - core) * half, half), :],
                acts[item, span(first + core * half, half), :],
            ],
            axis=0,
        )

        @pl.loop(0, hidden // tile_h)
        def _(n):
            at = span(n * tile_h, tile_h)
            if item == 0:
                part = contract(left, wi[:, at], 1, 0)
            else:
                part = contract(left, wo[at, :], 1, 1)
            pair_send[g, item, :, at] = part[:half]
            pair_own[g, item, :, at] = part[half:]

        pair_copy(g, item).start()
        pending.append(pair_copy(g, item))

    def pair_copy(g, item):
        return remote(
            pair_send.at[g, item], pair_recv.at[g, item],
            pair_s.at[g, item], pair_r.at[g, item], "row", partner,
        )

    def line_copy(g, off):
        return remote(
            line_send.at[g, off - 1], line_recv.at[g, off - 1],
            line_s.at[g, off], line_r.at[g, off], "row", line_peer(off),
        )

    def pair_sum(g):
        for item in range(2):
            pair_copy(g, item).wait_recv()
        for off in range(1, nx):
            take = span(lax.rem(x + off, nx) * piece, piece)
            for item in range(2):
                line_send[g, off - 1, item] = (
                    pair_own[g, item, take, :] + pair_recv[g, item, take, :]
                ).astype(jnp.bfloat16)
            line_copy(g, off).start()
            pending.append(line_copy(g, off))
        take = span(x * piece, piece)
        for item in range(2):
            line_own[g, item] = pair_own[g, item, take, :] + pair_recv[g, item, take, :]

    def gather_block(g, xs):
        return hd.at[:, span(order[g][0] * size + core * half + xs * piece, piece), :]

    def gather_copy(g, off):
        block = gather_block(g, x)
        return remote(
            block, block, gather_s.at[g, off], gather_r.at[g, off], "row", line_peer(off)
        )

    def active(g):
        for off in range(1, nx):
            line_copy(g, off).wait_recv()
        first = order[g][0] * size + core * half + x * piece

        @pl.loop(0, hidden // LANES)
        def _(n):
            at = span(n * LANES, LANES)
            preact, hidden_grad = line_own[g, 0, :, at], line_own[g, 1, :, at]
            for off in range(1, nx):
                preact = preact + line_recv[g, off - 1, 0, :, at].astype(jnp.float32)
                hidden_grad = hidden_grad + line_recv[g, off - 1, 1, :, at].astype(jnp.float32)
            value, slope = activate(preact, hidden_grad)
            hd[0, span(first, piece), at] = value
            hd[1, span(first, piece), at] = slope

        for off in range(1, nx):
            gather_copy(g, off).start()
            pending.append(gather_copy(g, off))

    def share_copy(g, which):
        block = hd.at[:, span(order[g][0] * size + which * half, half), :]
        return remote(block, block, share_s.at[g], share_r.at[g], "row", partner)

    def share(g):
        for off in range(1, nx):
            xs = lax.rem(x + nx - off, nx)
            block = gather_block(g, xs)
            remote(
                block, block, gather_s.at[g, off], gather_r.at[g, off], "row", line_peer(off)
            ).wait_recv()
        share_copy(g, core).start()
        pending.append(share_copy(g, core))

    def share_wait(g):
        share_copy(g, 1 - core).wait_recv()

    def dx_copy(g, off):
        return remote(
            dx_send.at[g, off - 1], dx_recv.at[g, off - 1],
            dy_s.at[g, off], dy_r.at[g, off], "col", y_peer(off),
        )

    def back_product(groups):
        left = jnp.concatenate(
            [
                hd[1, span(order[g][0] * size + lax.rem(y + off, ny) * t, t), :]
                for g in groups
                for off in range(ny)
            ],
            axis=0,
        )

        @pl.loop(0, width // tile_w)
        def _(n):
            at = span(n * tile_w, tile_w)
            part = contract(left, wi[at, :], 1, 1)
            for i, g in enumerate(groups):
                for off in range(ny):
                    low = (i * ny + off) * t
                    if off == 0:
                        dx_own[g, :, at] = part[low : low + t]
                    else:
                        dx_send[g, off - 1, :, at] = part[low : low + t].astype(jnp.bfloat16)

        for g in groups:
            for off in range(1, ny):
                dx_copy(g, off).start()
                pending.append(dx_copy(g, off))

    def dz_copy(g):
        return remote(
            dz_send.at[g], dz_recv.at[z], dz_s.at[g], dz_r.at[z], "col", order[g][0] * ny + y
        )

    def back_sum(g):
        for off in range(1, ny):
            dx_copy(g, off).wait_recv()
        total = dx_own[g]
        for off in range(1, ny):
            total = total + dx_recv[g, off - 1].astype(jnp.float32)
        if g == 0:
            dx_own[0] = total
        else:
            dz_send[g] = total.astype(jnp.bfloat16)
            dz_copy(g).start()
            pending.append(dz_copy(g))

    outs = []

    def put(source, target, slot):
        copy = pltpu.make_async_copy(source, target, out_sem.at[slot])
        copy.start()
        outs.append(copy)

    use_grams = grams is not None
    tile_t = 256 if tokens % 256 == 0 else 128

    def gram(which, source, item):
        @pl.loop(0, tokens // tile_t)
        def _(n):
            at = span(n * tile_t, tile_t)
            grams[which, :, at] = contract(source[item], source[item, at, :], 1, 1)

    def local_total():
        if use_grams:
            part_ref[...] = jnp.zeros_like(part_ref)

            @pl.loop(0, tokens // tile_t)
            def _(n):
                at = span(n * tile_t, tile_t)
                late_in = contract(hd[1], hd[1, at, :], 1, 1)
                part_ref[...] += folded(late_in * grams[0, :, at])
                late_out = contract(hd[0], hd[0, at, :], 1, 1)
                part_ref[...] += folded(late_out * grams[1, :, at])
        else:
            part_ref[...] = jnp.zeros_like(part_ref)
            for left, right, count in ((acts.at[0], hd.at[1], width), (hd.at[0], acts.at[1], hidden)):

                @pl.loop(0, count // LANES)
                def _(n):
                    at = span(n * LANES, LANES)
                    part = contract(left[:, at], right[...], 0, 0)
                    part_ref[...] += folded(part * part)

    for s in range(nz + 3):
        if s + 1 < nz:
            forward(s + 1)
        if s < nz:
            for item in range(2):
                y_wait(s, item)
                if s == 0:
                    loads[2 + item].wait()
                forward_product(s, item)
        if 0 <= s - 1 < nz:
            active(s - 1)
        if s == nz - 1:
            put(acts.at[0], x_out, 0)
            put(acts.at[1], c_out, 1)
        if s < nz:
            pair_sum(s)
        if s == nz and use_grams:
            gram(0, acts, 0)
            gram(1, acts, 1)
        if 0 <= s - 2 < nz:
            share(s - 2)
        if 0 <= s - 3 < nz:
            share_wait(s - 3)
        if s == nz - 1:
            back_product(list(range(nz - 3)))
        if s == nz:
            back_product([nz - 3])
            for g in range(nz - 3):
                back_sum(g)
        if s == nz + 1:
            back_product([nz - 2])
            back_sum(nz - 3)
    put(hd.at[0], hidden_out, 2)
    put(hd.at[1], delta_out, 3)
    back_product([nz - 1])
    local_total()

    def col_copy(off):
        return remote(
            part_ref, col_tops.at[off], tot_s.at[off], tot_r.at[off],
            "col", lax.rem(k + off, cols),
        )

    def row_copy(off):
        return remote(
            col_tops.at[0], row_tops.at[off], row_s.at[off], row_r.at[off],
            "row", lax.rem(r + off, rows),
        )

    for off in range(1, cols):
        col_copy(off).start()
        pending.append(col_copy(off))
    back_sum(nz - 2)
    back_sum(nz - 1)
    for off in range(1, cols):
        col_copy(off).wait_recv()
    total = part_ref[...]
    for off in range(1, cols):
        total = total + col_tops[off]
    col_tops[0] = total
    for off in range(1, rows):
        row_copy(off).start()
        pending.append(row_copy(off))
    for off in range(1, rows):
        row_copy(off).wait_recv()
        total = total + row_tops[off]
    total = jnp.sum(jnp.sum(total, axis=0, keepdims=True), axis=1, keepdims=True)
    total = jnp.maximum(total, 0.0)
    factor = 1.0 / jnp.maximum(jnp.sqrt(total / entries), 1.0)
    factor_ref[...] = jnp.broadcast_to(factor, factor_ref.shape)

    total = dx_own[0]
    for off in range(1, nz):
        zs = lax.rem(z + off, nz)
        remote(
            dz_send.at[1], dz_recv.at[zs], dz_s.at[1], dz_r.at[zs], "col", y_peer(1)
        ).wait_recv()
        total = total + dz_recv[zs].astype(jnp.float32)
    grad_ref[...] = total.astype(jnp.bfloat16)

    for item in range(2):
        for way, sign, there in ways:
            pl.when(there)(lambda i=item, w=way, s=sign: z_copy(i, z, 0, w, s).wait_send())
    for g in range(1, nz):
        zs, sign, there = onward(g)
        for item in range(2):
            pl.when(there)(lambda i=item, a=zs, b=g, s=sign: z_copy(i, a, b, 0, s).wait_send())
    for copy in pending:
        copy.wait_send()
    for copy in outs:
        copy.wait()


def front(sizes, inputs, cotangent, weight_in, weight_out):
    rows, cols = sizes["row"], sizes["col"]
    nx = rows // 2
    ny = 2 ** ((cols.bit_length() - 1) // 2)
    nz = cols // ny
    t, width = inputs.shape
    hidden = weight_in.shape[1]
    size = t * ny
    half, tokens = size // 2, size * nz
    piece = half // nx
    entries = 2.0 * width * rows * hidden * cols
    bf, f4 = jnp.bfloat16, jnp.float32
    use_grams = tokens <= hidden
    dma = lambda *dims: pltpu.SemaphoreType.DMA(dims)
    scratch = [
        pltpu.VMEM((2, tokens, width), bf),
        pltpu.VMEM(weight_in.shape, bf),
        pltpu.VMEM(weight_out.shape, bf),
        pltpu.VMEM((nz, 2, half, hidden), f4),
        pltpu.VMEM((nz, 2, half, hidden), f4),
        pltpu.VMEM((nz, 2, half, hidden), f4),
        pltpu.VMEM((nz, nx - 1, 2, piece, hidden), bf),
        pltpu.VMEM((nz, nx - 1, 2, piece, hidden), bf),
        pltpu.VMEM((nz, 2, piece, hidden), f4),
        pltpu.VMEM((2, tokens, hidden), bf),
        pltpu.VMEM((nz, t, width), f4),
        pltpu.VMEM((nz, ny - 1, t, width), bf),
        pltpu.VMEM((nz, ny - 1, t, width), bf),
        pltpu.VMEM((nz, t, width), bf),
        pltpu.VMEM((nz, t, width), bf),
        pltpu.VMEM((8, LANES), f4),
        pltpu.VMEM((cols, 8, LANES), f4),
        pltpu.VMEM((rows, 8, LANES), f4),
        pltpu.VMEM((2, tokens, tokens), f4) if use_grams else None,
        dma(4),
        dma(2, nz, 2), dma(2, nz), dma(2, nz, ny), dma(2, nz, ny),
        dma(nz, 2), dma(nz, 2), dma(nz, nx), dma(nz, nx),
        dma(nz, nx), dma(nz, nx), dma(nz), dma(nz),
        dma(nz, ny), dma(nz, ny), dma(nz), dma(nz),
        dma(cols), dma(cols), dma(rows), dma(rows), dma(4),
    ]
    kept = [item for item in scratch if item is not None]
    slot = 10 + scratch.index(None) if None in scratch else None

    def kernel(*refs):
        refs = list(refs)
        if slot is not None:
            refs.insert(slot, None)
        front_kernel((rows, cols, nx, ny, nz, entries), *refs)

    anywhere = pl.BlockSpec(memory_space=pl.ANY)
    inside = pl.BlockSpec(memory_space=pltpu.VMEM)
    return pl.pallas_call(
        kernel,
        out_shape=[
            jax.ShapeDtypeStruct((tokens, width), bf),
            jax.ShapeDtypeStruct((tokens, width), bf),
            jax.ShapeDtypeStruct((tokens, hidden), bf),
            jax.ShapeDtypeStruct((tokens, hidden), bf),
            jax.ShapeDtypeStruct((t, width), bf),
            jax.ShapeDtypeStruct((8, LANES), f4),
        ],
        in_specs=[anywhere] * 4,
        out_specs=[anywhere] * 4 + [inside] * 2,
        scratch_shapes=kept,
        compiler_params=pltpu.CompilerParams(
            collective_id=0, has_side_effects=True, vmem_limit_bytes=60 * 2**20
        ),
        name="front",
    )(inputs, cotangent, weight_in, weight_out)


def row_block(rows):
    return 256 if rows % 256 == 0 else 128


def to_lanes(column_tops):
    pieces = []
    for at in range(0, column_tops.shape[0], LANES):
        turned = column_tops[at : at + LANES].T
        pieces.append(jnp.max(turned, axis=0, keepdims=True))
    return jnp.concatenate(pieces, axis=1)


def lane_fold(values, combine):
    top = values[:, :LANES]
    for at in range(LANES, values.shape[1], LANES):
        top = combine(top, values[:, at : at + LANES])
    return top


def sublane_fold(values, combine):
    top = values[:PACKED]
    for low in range(PACKED, values.shape[0], PACKED):
        top = combine(top, values[low : low + PACKED])
    return top


second_gain = ((1.0 - second_decay) / second_decay) ** 0.5
moment_gain = (1.0 - momentum_decay) / momentum_decay / second_gain
root_gain = second_decay**0.5 / momentum_decay


def moments_block(at, gain, left_ref, right_ref, sources, targets, row_ref, row_at, col_ref, turned):
    weight_ref, moment_ref, second_ref = sources
    new_moment_ref, new_second_ref = targets
    block, width = turned.shape[0], weight_ref.shape[1]
    rows = span(at * block, block)
    turned[:, :] = left_ref[:, rows].T
    tile = 256 if width % 256 == 0 else 128
    row_tops = [None, None]
    for low in range(0, width, tile):
        take = slice(low, low + tile)
        pulled = contract(turned[...], right_ref[:, take], 1, 0) * gain
        moment = moment_ref[rows, take] + (pulled * moment_gain).astype(jnp.bfloat16)
        second = second_ref[rows, take] + (pulled * pulled).astype(jnp.bfloat16)
        wide = second.astype(jnp.float32)
        root = wide * lax.rsqrt(wide)
        step = moment.astype(jnp.float32) / (root * root_gain + stable_eps / momentum_decay)
        decayed = weight_ref[rows, take] * jnp.bfloat16(weight_decay)
        weight_ref[rows, take] = step.astype(jnp.bfloat16) + decayed
        new_moment_ref[rows, take] = moment
        new_second_ref[rows, take] = second
        for which, value in enumerate((jnp.abs(moment), second)):
            top = lane_fold(value, jnp.maximum)
            row_tops[which] = top if low == 0 else jnp.maximum(row_tops[which], top)
            col_ref[which, :, take] = jnp.maximum(
                col_ref[which, :, take], sublane_fold(value, jnp.maximum)
            )
    for which in range(2):
        row_ref[row_at + which : row_at + which + 1, rows] = to_lanes(
            row_tops[which].astype(jnp.float32)
        )


def moments_kernel(
    factor_ref, inputs_hbm, delta_hbm, hidden_hbm, cotangent_hbm,
    weight_in_hbm, moment_in_hbm, second_in_hbm, weight_out_hbm, moment_out_hbm, second_out_hbm,
    update_in, update_out, new_moment_in, new_second_in, new_moment_out, new_second_out,
    by_col, by_row,
    inputs, delta, hidden, cotangent,
    weight_in, moment_in, second_in, weight_out, moment_out, second_out,
    cols_in, cols_out, turned_in, turned_out, side_sem, in_sem, out_sem, put_in, put_out,
):
    block_in, block_out = turned_in.shape[0], turned_out.shape[0]
    steps_in, steps_out = weight_in.shape[0] // block_in, weight_out.shape[0] // block_out
    sides = [
        pltpu.make_async_copy(source, target, side_sem.at[at])
        for at, (source, target) in enumerate(
            (
                (inputs_hbm, inputs), (delta_hbm, delta),
                (hidden_hbm, hidden), (cotangent_hbm, cotangent),
            )
        )
    ]
    pairs_in = (
        (weight_in_hbm, weight_in), (moment_in_hbm, moment_in), (second_in_hbm, second_in)
    )
    pairs_out = (
        (weight_out_hbm, weight_out), (moment_out_hbm, moment_out), (second_out_hbm, second_out)
    )

    def loads(pairs, sems, block, at):
        rows = span(at * block, block)
        return [
            pltpu.make_async_copy(source.at[rows, :], target.at[rows, :], sems.at[which, at])
            for which, (source, target) in enumerate(pairs)
        ]

    def begin_in(at):
        for copy in loads(pairs_in, in_sem, block_in, at):
            copy.start()

    def begin_out(at):
        for copy in loads(pairs_out, out_sem, block_out, at):
            copy.start()

    def put(source, target, sems, block, at):
        rows = span(at * block, block)
        return pltpu.make_async_copy(source.at[rows, :], target.at[rows, :], sems.at[at])

    sides[0].start()
    sides[1].start()
    for at in range(AHEAD):
        begin_in(at)
    cols_in[...] = jnp.zeros_like(cols_in)
    cols_out[...] = jnp.zeros_like(cols_out)
    gain = factor_ref[0:1, 0:1] * second_gain
    sides[0].wait()
    sides[1].wait()
    sides[2].start()
    sides[3].start()

    @pl.loop(0, steps_in)
    def _(at):
        pl.when(at + AHEAD < steps_in)(lambda: begin_in(at + AHEAD))
        pl.when(at + AHEAD >= steps_in)(lambda: begin_out(at + AHEAD - steps_in))
        for copy in loads(pairs_in, in_sem, block_in, at):
            copy.wait()
        moments_block(
            at, gain, inputs, delta, (weight_in, moment_in, second_in),
            (new_moment_in, new_second_in), by_col, 0, cols_in, turned_in,
        )
        put(weight_in, update_in, put_in, block_in, at).start()

    sides[2].wait()
    sides[3].wait()

    @pl.loop(0, steps_out)
    def _(at):
        pl.when(at + AHEAD < steps_out)(lambda: begin_out(at + AHEAD))
        for copy in loads(pairs_out, out_sem, block_out, at):
            copy.wait()
        moments_block(
            at, gain, hidden, cotangent, (weight_out, moment_out, second_out),
            (new_moment_out, new_second_out), by_row, 2, cols_out, turned_out,
        )
        put(weight_out, update_out, put_out, block_out, at).start()

    for which in range(2):
        top = cols_in[which].astype(jnp.float32)
        by_row[which : which + 1, :] = jnp.max(top, axis=0, keepdims=True)
        top = cols_out[which].astype(jnp.float32)
        by_col[which + 2 : which + 3, :] = jnp.max(top, axis=0, keepdims=True)
    for at in range(steps_in):
        put(weight_in, update_in, put_in, block_in, at).wait()
    for at in range(steps_out):
        put(weight_out, update_out, put_out, block_out, at).wait()


def held(shape):
    return pltpu.VMEM(shape, jnp.bfloat16)


def moments(factor, inputs, delta, hidden, cotangent, first, latter):
    width, units = first[0].shape
    tokens = inputs.shape[0]
    block_in, block_out = row_block(width), row_block(units)
    steps_in, steps_out = width // block_in, units // block_out
    inside = pl.BlockSpec(memory_space=pltpu.VMEM)
    anywhere = pl.BlockSpec(memory_space=pl.ANY)
    return pl.pallas_call(
        moments_kernel,
        out_shape=[
            jax.ShapeDtypeStruct((width, units), jnp.bfloat16),
            jax.ShapeDtypeStruct((units, width), jnp.bfloat16),
            held((width, units)),
            held((width, units)),
            held((units, width)),
            held((units, width)),
            jax.ShapeDtypeStruct((4, width), jnp.float32),
            jax.ShapeDtypeStruct((4, units), jnp.float32),
        ],
        in_specs=[inside] + [anywhere] * 10,
        out_specs=[anywhere] * 2 + [inside] * 6,
        scratch_shapes=[
            held((tokens, width)),
            held((tokens, units)),
            held((tokens, units)),
            held((tokens, width)),
        ]
        + [held((width, units))] * 3
        + [held((units, width))] * 3
        + [
            held((2, PACKED, units)),
            held((2, PACKED, width)),
            held((block_in, tokens)),
            held((block_out, tokens)),
            pltpu.SemaphoreType.DMA((4,)),
            pltpu.SemaphoreType.DMA((3, steps_in)),
            pltpu.SemaphoreType.DMA((3, steps_out)),
            pltpu.SemaphoreType.DMA((steps_in,)),
            pltpu.SemaphoreType.DMA((steps_out,)),
        ],
        compiler_params=pltpu.CompilerParams(vmem_limit_bytes=VMEM_MOMENTS),
        name="moments",
    )(factor, inputs, delta, hidden, cotangent, *first, *latter)


def tops_kernel(sizes, col_ref, row_ref, all_col, all_row, send_c, recv_c, send_r, recv_r):
    jobs = (
        ("col", col_ref, all_col, send_c, recv_c),
        ("row", row_ref, all_row, send_r, recv_r),
    )
    barrier = pltpu.get_barrier_semaphore()
    for axis, *_ in jobs:
        me = lax.axis_index(axis)
        for off in range(1, sizes[axis]):
            peer = lax.rem(me + off, sizes[axis])
            pl.semaphore_signal(barrier, inc=1, device_id={axis: peer}, device_id_type=MESH)
    pl.semaphore_wait(barrier, sizes["col"] + sizes["row"] - 2)
    copies = []
    for axis, source, target, send, receive in jobs:
        me = lax.axis_index(axis)
        for off in range(1, sizes[axis]):
            peer = lax.rem(me + off, sizes[axis])
            copy = remote(source, target.at[off], send.at[off], receive.at[off], axis, peer)
            copy.start()
            copies.append(copy)
    for _, source, target, *_ in jobs:
        target[0] = source[...]
    for copy in copies:
        copy.wait()


def exchange_tops(sizes, by_col, by_row):
    rows, cols = sizes["row"], sizes["col"]
    inside = pl.BlockSpec(memory_space=pltpu.VMEM)
    return pl.pallas_call(
        functools.partial(tops_kernel, sizes),
        out_shape=[
            jax.ShapeDtypeStruct((cols,) + by_col.shape, jnp.float32),
            jax.ShapeDtypeStruct((rows,) + by_row.shape, jnp.float32),
        ],
        in_specs=[inside] * 2,
        out_specs=[inside] * 2,
        scratch_shapes=[
            pltpu.SemaphoreType.DMA((cols,)),
            pltpu.SemaphoreType.DMA((cols,)),
            pltpu.SemaphoreType.DMA((rows,)),
            pltpu.SemaphoreType.DMA((rows,)),
        ],
        compiler_params=pltpu.CompilerParams(
            collective_id=1, has_side_effects=True, vmem_limit_bytes=4 * 2**20
        ),
        name="tops",
    )(by_col, by_row)


def encode_block(at, block, sources, targets, row_ref, row_at, col_ref, col_at):
    cols = targets[0].shape[1]
    for which in range(2):
        source, target = sources[which], targets[which]
        for low in range(0, block, LANES):
            rows = span(at * block + low, LANES)
            inverse = row_ref[row_at + which : row_at + which + 1, rows]
            inverse = jnp.broadcast_to(inverse, (LANES, LANES)).T
            for lane in range(0, cols, LANES):
                other = col_ref[col_at + which : col_at + which + 1, lane : lane + LANES]
                value = source[rows, lane : lane + LANES].astype(jnp.float32)
                value = value * jnp.maximum(inverse, other)
                target[rows, lane : lane + LANES] = value.astype(jnp.bfloat16)


def encode_kernel(
    all_col, all_row, moment_in, second_in, moment_out, second_out,
    code_moment_in, code_second_in, code_moment_out, code_second_out,
    row_scale_in, col_scale_in, row_scale_out, col_scale_out,
    inverse_col, inverse_row, made_moment_in, made_second_in, made_moment_out, made_second_out,
    in_sem, out_sem,
):
    for source, inverse, scales in (
        (all_col, inverse_col, (row_scale_in, col_scale_out)),
        (all_row, inverse_row, (col_scale_in, row_scale_out)),
    ):
        top = source[0]
        for at in range(1, source.shape[0]):
            top = jnp.maximum(top, source[at])
        for at in range(4):
            decay = second_decay if at % 2 else momentum_decay
            scale = jnp.maximum(top[at : at + 1] * decay, 1.0)
            scales[at // 2][at % 2 : at % 2 + 1, :] = scale
            inverse[at : at + 1, :] = decay / scale

    jobs = (
        (
            (moment_in, second_in), (made_moment_in, made_second_in),
            (code_moment_in, code_second_in), inverse_col, 0, inverse_row, 0, in_sem,
        ),
        (
            (moment_out, second_out), (made_moment_out, made_second_out),
            (code_moment_out, code_second_out), inverse_row, 2, inverse_col, 2, out_sem,
        ),
    )

    def puts(made, codes, sems, block, at):
        rows = span(at * block, block)
        return [
            pltpu.make_async_copy(made[i].at[rows, :], codes[i].at[rows, :], sems.at[i, at])
            for i in range(2)
        ]

    for sources, made, codes, row_ref, row_at, col_ref, col_at, sems in jobs:
        block = row_block(made[0].shape[0])

        @pl.loop(0, made[0].shape[0] // block)
        def _(at):
            encode_block(at, block, sources, made, row_ref, row_at, col_ref, col_at)
            for copy in puts(made, codes, sems, block, at):
                copy.start()

    for sources, made, codes, row_ref, row_at, col_ref, col_at, sems in jobs:
        block = row_block(made[0].shape[0])
        for at in range(made[0].shape[0] // block):
            for copy in puts(made, codes, sems, block, at):
                copy.wait()


def encode(all_col, all_row, moment_in, second_in, moment_out, second_out):
    width, units = moment_in.shape
    inside = pl.BlockSpec(memory_space=pltpu.VMEM)
    anywhere = pl.BlockSpec(memory_space=pl.ANY)
    half, full = jnp.bfloat16, jnp.float32
    return pl.pallas_call(
        encode_kernel,
        out_shape=[
            jax.ShapeDtypeStruct((width, units), half),
            jax.ShapeDtypeStruct((width, units), half),
            jax.ShapeDtypeStruct((units, width), half),
            jax.ShapeDtypeStruct((units, width), half),
            jax.ShapeDtypeStruct((2, width), full),
            jax.ShapeDtypeStruct((2, units), full),
            jax.ShapeDtypeStruct((2, units), full),
            jax.ShapeDtypeStruct((2, width), full),
        ],
        in_specs=[inside] * 6,
        out_specs=[anywhere] * 4 + [inside] * 4,
        scratch_shapes=[
            pltpu.VMEM((4, width), full),
            pltpu.VMEM((4, units), full),
            pltpu.VMEM((width, units), half),
            pltpu.VMEM((width, units), half),
            pltpu.VMEM((units, width), half),
            pltpu.VMEM((units, width), half),
            pltpu.SemaphoreType.DMA((2, width // row_block(width))),
            pltpu.SemaphoreType.DMA((2, units // row_block(units))),
        ],
        compiler_params=pltpu.CompilerParams(vmem_limit_bytes=VMEM_ENCODE),
        name="encode",
    )(
        all_col,
        all_row,
        *(
            pltpu.with_memory_space_constraint(value, pltpu.VMEM)
            for value in (moment_in, second_in, moment_out, second_out)
        ),
    )


def shards(
    sizes, inputs, cotangent, weight_in, moment_in, second_in, weight_out, moment_out, second_out
):
    all_inputs, all_cotangent, all_hidden, all_delta, input_grad, factor = front(
        sizes, inputs, cotangent, weight_in, weight_out
    )
    update_in, update_out, *kept, by_col, by_row = moments(
        factor,
        all_inputs,
        all_delta,
        all_hidden,
        all_cotangent,
        (weight_in, moment_in, second_in),
        (weight_out, moment_out, second_out),
    )
    all_col, all_row = exchange_tops(sizes, by_col, by_row)
    (
        code_moment_in, code_second_in, code_moment_out, code_second_out,
        rows_in, cols_in, rows_out, cols_out,
    ) = encode(all_col, all_row, *kept)
    return (
        input_grad,
        update_in,
        code_moment_in,
        code_second_in,
        rows_in,
        cols_in,
        update_out,
        code_moment_out,
        code_second_out,
        rows_out,
        cols_out,
    )


def solution(mesh):
    in_specs = (
        P("col", "row"),
        P("col", "row"),
        P("row", "col"),
        P("row", "col"),
        P("row", "col"),
        P("col", "row"),
        P("col", "row"),
        P("col", "row"),
    )
    out_specs = (
        P("col", "row"),
        P("row", "col"),
        P("row", "col"),
        P("row", "col"),
        P(None, "row"),
        P(None, "col"),
        P("col", "row"),
        P("col", "row"),
        P("col", "row"),
        P(None, "col"),
        P(None, "row"),
    )
    sizes = {axis: mesh.shape[axis] for axis in ("row", "col")}
    return jax.shard_map(
        functools.partial(shards, sizes),
        mesh=mesh,
        in_specs=in_specs,
        out_specs=out_specs,
        check_vma=False,
    )
```

```python
import functools

import jax
import jax.numpy as jnp
from jax import lax
from jax.experimental import pallas as pl
from jax.experimental.pallas import tpu as pltpu
from jax.sharding import PartitionSpec as P

root_half = 0.7071067811865476
normal_density = 0.3989422804014327
momentum_decay = 0.9
second_decay = 0.95
stable_eps = 1e-08
weight_decay = 0.1
LANES = 128
PACKED = 16
AHEAD = 2
VMEM_MOMENTS = 40 * 2**20
VMEM_ENCODE = 40 * 2**20


def contract(left, right, left_dim, right_dim):
    return lax.dot_general(
        left, right, (((left_dim,), (right_dim,)), ((), ())), preferred_element_type=jnp.float32
    )


def activate(preact, hidden_grad):
    cumulative = 0.5 * (1.0 + lax.erf(preact * root_half))
    density = jnp.exp(-0.5 * preact * preact) * normal_density
    hidden = (preact * cumulative).astype(jnp.bfloat16)
    delta = (hidden_grad * (cumulative + preact * density)).astype(jnp.bfloat16)
    return (hidden, delta)


MESH = pl.DeviceIdType.MESH


def remote(source, target, send, receive, axis, peer):
    return pltpu.make_async_remote_copy(
        src_ref=source,
        dst_ref=target,
        send_sem=send,
        recv_sem=receive,
        device_id={axis: peer},
        device_id_type=MESH,
    )


def span(start, size):
    return pl.ds(pl.multiple_of(start, size), size)


def lane_tile(size):
    return 512 if size % 512 == 0 else 256 if size % 256 == 0 else 128


def folded(values):
    total = values[:8, :LANES] * 0.0
    for low in range(0, values.shape[0], 8):
        for at in range(0, values.shape[1], LANES):
            total = total + values[low : low + 8, at : at + LANES]
    return total


def front_kernel(
    shape, x_ref, c_ref, wi_hbm, wo_hbm,
    x_out, c_out, hidden_out, delta_out, grad_ref, factor_ref,
    acts, wi, wo, pair_send, pair_recv, pair_own, line_send, line_recv, line_own, hd,
    dx_own, dx_send, dx_recv, dz_send, dz_recv, part_ref, col_tops, row_tops, grams,
    load_sem, z_send, z_recv, y_send, y_recv, pair_s, pair_r, line_s, line_r,
    gather_s, gather_r, share_s, share_r, dy_s, dy_r, dz_s, dz_r,
    tot_s, tot_r, row_s, row_r, out_sem,
):
    rows, cols, nx, ny, nz, entries = shape
    t, width = x_ref.shape
    hidden = wi.shape[1]
    size = ny * t
    half = t // 2
    piece = half // nx
    tokens = size * nz
    r, k = lax.axis_index("row"), lax.axis_index("col")
    x, core = r // 2, r % 2
    z, y = k // ny, k % ny
    partner = x * 2 + (1 - core)
    below, above = z, nz - 1 - z
    middle = jnp.minimum(below, above)

    def source_of(g):
        if g == 0:
            return z, 0
        near = g <= 2 * middle
        distance = jnp.where(near, (g + 1) // 2, g - middle)
        side = jnp.where(near, -1 if g % 2 else 1, jnp.where(above > below, 1, -1))
        return z + side * distance, side

    order = [source_of(g) for g in range(nz)]

    def line_peer(off):
        return lax.rem(x + off, nx) * 2 + core

    def y_peer(off):
        return z * ny + lax.rem(y + off, ny)

    loads = [
        pltpu.make_async_copy(x_ref, acts.at[0, span(k * t, t)], load_sem.at[0]),
        pltpu.make_async_copy(c_ref, acts.at[1, span(k * t, t)], load_sem.at[1]),
        pltpu.make_async_copy(wi_hbm, wi, load_sem.at[2]),
        pltpu.make_async_copy(wo_hbm, wo, load_sem.at[3]),
    ]
    for load in loads:
        load.start()
    barrier = pltpu.get_barrier_semaphore()
    for off in range(1, cols):
        pl.semaphore_signal(
            barrier, inc=1, device_id={"col": lax.rem(k + off, cols)}, device_id_type=MESH
        )
    for off in range(1, rows):
        pl.semaphore_signal(
            barrier, inc=1, device_id={"row": lax.rem(r + off, rows)}, device_id_type=MESH
        )
    loads[0].wait()
    loads[1].wait()
    pl.semaphore_wait(barrier, cols + rows - 2)

    pending = []

    def z_copy(item, zs, g, way, sign):
        block = acts.at[item, span((zs * ny + y) * t, t)]
        return remote(
            block, block, z_send.at[item, g, way], z_recv.at[item, zs], "col", (z + sign) * ny + y
        )

    def y_copies(item, zs, g):
        block = acts.at[item, span((zs * ny + y) * t, t)]
        copies = [
            remote(
                block, block, y_send.at[item, g, off], y_recv.at[item, zs, y], "col", y_peer(off)
            )
            for off in range(1, ny)
        ]
        for copy in copies:
            copy.start()
            pending.append(copy)

    ways = ((0, 1, z < nz - 1), (1, -1, z > 0))
    for item in range(2):
        for way, sign, there in ways:
            pl.when(there)(lambda i=item, w=way, s=sign: z_copy(i, z, 0, w, s).start())
        y_copies(item, z, 0)

    def onward(g):
        zs, side = order[g]
        ahead = z - side
        return zs, -side, jnp.logical_and(ahead >= 0, ahead < nz)

    def forward(g):
        zs, sign, there = onward(g)
        for item in range(2):
            block = acts.at[item, span((zs * ny + y) * t, t)]
            remote(
                block, block, z_send.at[item, g, 0], z_recv.at[item, zs], "col", y_peer(1)
            ).wait_recv()
            pl.when(there)(lambda i=item: z_copy(i, zs, g, 0, sign).start())
            y_copies(item, zs, g)

    def first_row(unit):
        g, j = unit
        return (order[g][0] * ny + lax.rem(y + j, ny)) * t

    def y_wait(g, item):
        zs, _ = order[g]
        for off in range(1, ny):
            ys = lax.rem(y + off, ny)
            block = acts.at[item, span((zs * ny + ys) * t, t)]
            remote(
                block, block, y_send.at[item, g, off], y_recv.at[item, zs, ys], "col", y_peer(1)
            ).wait_recv()

    tile_h, tile_w = lane_tile(hidden), lane_tile(width)
    chunks = width // tile_w

    def forward_product(units, item):
        left = jnp.concatenate(
            [
                acts[item, span(first_row(unit) + which * half, half), :]
                for unit in units
                for which in (1 - core, core)
            ],
            axis=0,
        )

        @pl.loop(0, hidden // tile_h)
        def _(n):
            at = span(n * tile_h, tile_h)
            if item == 0:
                part = contract(left, wi[:, at], 1, 0)
            else:
                part = contract(left, wo[at, :], 1, 1)
            for i, (g, j) in enumerate(units):
                low = i * t
                pair_send[g, j, item, :, at] = part[low : low + half]
                pair_own[g, j, item, :, at] = part[low + half : low + t]

        for unit in units:
            pair_copy(unit, item).start()
            pending.append(pair_copy(unit, item))

    def pair_copy(unit, item):
        g, j = unit
        return remote(
            pair_send.at[g, j, item], pair_recv.at[g, j, item],
            pair_s.at[item, g, j], pair_r.at[item, g, j], "row", partner,
        )

    def line_copy(unit, off):
        g, j = unit
        return remote(
            line_send.at[g, j, off - 1], line_recv.at[g, j, off - 1],
            line_s.at[g, j, off], line_r.at[g, j, off], "row", line_peer(off),
        )

    def pair_sum(unit):
        g, j = unit
        for item in range(2):
            pair_copy(unit, item).wait_recv()
        for off in range(1, nx):
            take = span(lax.rem(x + off, nx) * piece, piece)
            for item in range(2):
                line_send[g, j, off - 1, item] = (
                    pair_own[g, j, item, take, :] + pair_recv[g, j, item, take, :]
                ).astype(jnp.bfloat16)
            line_copy(unit, off).start()
            pending.append(line_copy(unit, off))
        take = span(x * piece, piece)
        for item in range(2):
            line_own[g, j, item] = pair_own[g, j, item, take, :] + pair_recv[g, j, item, take, :]

    def gather_block(unit, xs):
        return hd.at[:, span(first_row(unit) + core * half + xs * piece, piece), :]

    def gather_copy(unit, off):
        g, j = unit
        block = gather_block(unit, x)
        return remote(
            block, block, gather_s.at[g, j, off], gather_r.at[g, j, off], "row", line_peer(off)
        )

    def active(unit):
        g, j = unit
        for off in range(1, nx):
            line_copy(unit, off).wait_recv()
        first = first_row(unit) + core * half + x * piece

        @pl.loop(0, hidden // LANES)
        def _(n):
            at = span(n * LANES, LANES)
            preact, hidden_grad = line_own[g, j, 0, :, at], line_own[g, j, 1, :, at]
            for off in range(1, nx):
                preact = preact + line_recv[g, j, off - 1, 0, :, at].astype(jnp.float32)
                hidden_grad = hidden_grad + line_recv[g, j, off - 1, 1, :, at].astype(jnp.float32)
            value, slope = activate(preact, hidden_grad)
            hd[0, span(first, piece), at] = value
            hd[1, span(first, piece), at] = slope

        for off in range(1, nx):
            gather_copy(unit, off).start()
            pending.append(gather_copy(unit, off))

    def share_copy(unit, which):
        block = hd.at[:, span(first_row(unit) + which * half, half), :]
        return remote(block, block, share_s.at[unit], share_r.at[unit], "row", partner)

    def share(unit):
        g, j = unit
        for off in range(1, nx):
            block = gather_block(unit, lax.rem(x + nx - off, nx))
            remote(
                block, block, gather_s.at[g, j, off], gather_r.at[g, j, off],
                "row", line_peer(off),
            ).wait_recv()
        share_copy(unit, core).start()
        pending.append(share_copy(unit, core))

    def share_wait(unit):
        share_copy(unit, 1 - core).wait_recv()

    def dx_copy(g, off, chunk):
        return remote(
            dx_send.at[g, off - 1, chunk], dx_recv.at[g, off - 1, chunk],
            dy_s.at[g, off, chunk], dy_r.at[g, off, chunk], "col", y_peer(off),
        )

    def back_product(batches):
        units = [unit for at in batches for unit in groups[at]]
        left = jnp.concatenate([hd[1, span(first_row(unit), t), :] for unit in units], axis=0)
        for chunk in range(chunks):
            part = contract(left, wi[chunk * tile_w : (chunk + 1) * tile_w, :], 1, 1)
            for i, (g, j) in enumerate(units):
                rows_of = part[i * t : (i + 1) * t]
                if j == 0:
                    dx_own[g, chunk] = rows_of
                else:
                    dx_send[g, j - 1, chunk] = rows_of.astype(jnp.bfloat16)
                    dx_copy(g, j, chunk).start()
                    pending.append(dx_copy(g, j, chunk))

    def dz_copy(g, chunk):
        return remote(
            dz_send.at[g, chunk], dz_recv.at[z, chunk], dz_s.at[g, chunk], dz_r.at[z, chunk],
            "col", order[g][0] * ny + y,
        )

    def back_sum(g):
        for chunk in range(chunks):
            total = dx_own[g, chunk]
            for off in range(1, ny):
                dx_copy(g, off, chunk).wait_recv()
                total = total + dx_recv[g, off - 1, chunk].astype(jnp.float32)
            if g == 0:
                dx_own[0, chunk] = total
            else:
                dz_send[g, chunk] = total.astype(jnp.bfloat16)
                dz_copy(g, chunk).start()
                pending.append(dz_copy(g, chunk))

    outs = []

    def put(source, target, slot):
        copy = pltpu.make_async_copy(source, target, out_sem.at[slot])
        copy.start()
        outs.append(copy)

    use_grams = grams is not None
    tile_t = 256 if tokens % 256 == 0 else 128

    def gram(which, source, item):
        @pl.loop(0, tokens // tile_t)
        def _(n):
            at = span(n * tile_t, tile_t)
            grams[which, :, at] = contract(source[item], source[item, at, :], 1, 1)

    def local_total():
        if use_grams:
            part_ref[...] = jnp.zeros_like(part_ref)

            @pl.loop(0, tokens // tile_t)
            def _(n):
                at = span(n * tile_t, tile_t)
                late_in = contract(hd[1], hd[1, at, :], 1, 1)
                part_ref[...] += folded(late_in * grams[0, :, at])
                late_out = contract(hd[0], hd[0, at, :], 1, 1)
                part_ref[...] += folded(late_out * grams[1, :, at])
        else:
            part_ref[...] = jnp.zeros_like(part_ref)
            for left, right, count in ((acts.at[0], hd.at[1], width), (hd.at[0], acts.at[1], hidden)):

                @pl.loop(0, count // LANES)
                def _(n):
                    at = span(n * LANES, LANES)
                    part = contract(left[:, at], right[...], 0, 0)
                    part_ref[...] += folded(part * part)

    others = range(1, ny)
    groups = [[(0, 0)]]
    groups += [[(g - 1, j) for j in others] + [(g, 0)] for g in range(1, nz)]
    groups += [[(nz - 1, j) for j in others]]

    for s in range(nz + 4):
        if 1 <= s < nz:
            forward(s)
        if s <= nz:
            for item in range(2):
                if s >= 1:
                    y_wait(s - 1, item)
                else:
                    loads[2 + item].wait()
                forward_product(groups[s], item)
        if s == nz:
            put(acts.at[0], x_out, 0)
            put(acts.at[1], c_out, 1)
        if 0 <= s - 1 <= nz:
            for unit in groups[s - 1]:
                active(unit)
        if s <= nz:
            for unit in groups[s]:
                pair_sum(unit)
        if s == nz + 1 and use_grams:
            gram(0, acts, 0)
            gram(1, acts, 1)
        if 0 <= s - 2 <= nz:
            for unit in groups[s - 2]:
                share(unit)
        if 0 <= s - 3 <= nz:
            for unit in groups[s - 3]:
                share_wait(unit)
        if s == nz:
            back_product(list(range(nz - 2)))
        if s == nz + 1:
            back_product([nz - 2])
            for g in range(nz - 3):
                back_sum(g)
        if s == nz + 2:
            back_product([nz - 1])
            back_sum(nz - 3)
    put(hd.at[0], hidden_out, 2)
    put(hd.at[1], delta_out, 3)
    back_product([nz])
    local_total()

    def col_copy(off):
        return remote(
            part_ref, col_tops.at[off], tot_s.at[off], tot_r.at[off],
            "col", lax.rem(k + off, cols),
        )

    def row_copy(off):
        return remote(
            col_tops.at[0], row_tops.at[off], row_s.at[off], row_r.at[off],
            "row", lax.rem(r + off, rows),
        )

    for off in range(1, cols):
        col_copy(off).start()
        pending.append(col_copy(off))
    back_sum(nz - 2)
    back_sum(nz - 1)
    for off in range(1, cols):
        col_copy(off).wait_recv()
    total = part_ref[...]
    for off in range(1, cols):
        total = total + col_tops[off]
    col_tops[0] = total
    for off in range(1, rows):
        row_copy(off).start()
        pending.append(row_copy(off))
    for off in range(1, rows):
        row_copy(off).wait_recv()
        total = total + row_tops[off]
    total = jnp.sum(jnp.sum(total, axis=0, keepdims=True), axis=1, keepdims=True)
    total = jnp.maximum(total, 0.0)
    factor = 1.0 / jnp.maximum(jnp.sqrt(total / entries), 1.0)
    factor_ref[...] = jnp.broadcast_to(factor, factor_ref.shape)

    for chunk in range(chunks):
        total = dx_own[0, chunk]
        for off in range(1, nz):
            zs = lax.rem(z + off, nz)
            remote(
                dz_send.at[1, chunk], dz_recv.at[zs, chunk],
                dz_s.at[1, chunk], dz_r.at[zs, chunk], "col", y_peer(1),
            ).wait_recv()
            total = total + dz_recv[zs, chunk].astype(jnp.float32)
        grad_ref[:, chunk * tile_w : (chunk + 1) * tile_w] = total.astype(jnp.bfloat16)

    for item in range(2):
        for way, sign, there in ways:
            pl.when(there)(lambda i=item, w=way, s=sign: z_copy(i, z, 0, w, s).wait_send())
    for g in range(1, nz):
        zs, sign, there = onward(g)
        for item in range(2):
            pl.when(there)(lambda i=item, a=zs, b=g, s=sign: z_copy(i, a, b, 0, s).wait_send())
    for copy in pending:
        copy.wait_send()
    for copy in outs:
        copy.wait()


def front(sizes, inputs, cotangent, weight_in, weight_out):
    rows, cols = sizes["row"], sizes["col"]
    nx = rows // 2
    ny = 2 ** ((cols.bit_length() - 1) // 2)
    nz = cols // ny
    t, width = inputs.shape
    hidden = weight_in.shape[1]
    size = t * ny
    half, tokens = t // 2, size * nz
    piece = half // nx
    tile = lane_tile(width)
    parts = (width // tile, t, tile)
    entries = 2.0 * width * rows * hidden * cols
    bf, f4 = jnp.bfloat16, jnp.float32
    use_grams = tokens <= hidden
    dma = lambda *dims: pltpu.SemaphoreType.DMA(dims)
    scratch = [
        pltpu.VMEM((2, tokens, width), bf),
        pltpu.VMEM(weight_in.shape, bf),
        pltpu.VMEM(weight_out.shape, bf),
        pltpu.VMEM((nz, ny, 2, half, hidden), f4),
        pltpu.VMEM((nz, ny, 2, half, hidden), f4),
        pltpu.VMEM((nz, ny, 2, half, hidden), f4),
        pltpu.VMEM((nz, ny, nx - 1, 2, piece, hidden), bf),
        pltpu.VMEM((nz, ny, nx - 1, 2, piece, hidden), bf),
        pltpu.VMEM((nz, ny, 2, piece, hidden), f4),
        pltpu.VMEM((2, tokens, hidden), bf),
        pltpu.VMEM((nz,) + parts, f4),
        pltpu.VMEM((nz, ny - 1) + parts, bf),
        pltpu.VMEM((nz, ny - 1) + parts, bf),
        pltpu.VMEM((nz,) + parts, bf),
        pltpu.VMEM((nz,) + parts, bf),
        pltpu.VMEM((8, LANES), f4),
        pltpu.VMEM((cols, 8, LANES), f4),
        pltpu.VMEM((rows, 8, LANES), f4),
        pltpu.VMEM((2, tokens, tokens), f4) if use_grams else None,
        dma(4),
        dma(2, nz, 2), dma(2, nz), dma(2, nz, ny), dma(2, nz, ny),
        dma(2, nz, ny), dma(2, nz, ny), dma(nz, ny, nx), dma(nz, ny, nx),
        dma(nz, ny, nx), dma(nz, ny, nx), dma(nz, ny), dma(nz, ny),
        dma(nz, ny, parts[0]), dma(nz, ny, parts[0]), dma(nz, parts[0]), dma(nz, parts[0]),
        dma(cols), dma(cols), dma(rows), dma(rows), dma(4),
    ]
    kept = [item for item in scratch if item is not None]
    slot = 10 + scratch.index(None) if None in scratch else None

    def kernel(*refs):
        refs = list(refs)
        if slot is not None:
            refs.insert(slot, None)
        front_kernel((rows, cols, nx, ny, nz, entries), *refs)

    anywhere = pl.BlockSpec(memory_space=pl.ANY)
    inside = pl.BlockSpec(memory_space=pltpu.VMEM)
    return pl.pallas_call(
        kernel,
        out_shape=[
            jax.ShapeDtypeStruct((tokens, width), bf),
            jax.ShapeDtypeStruct((tokens, width), bf),
            jax.ShapeDtypeStruct((tokens, hidden), bf),
            jax.ShapeDtypeStruct((tokens, hidden), bf),
            jax.ShapeDtypeStruct((t, width), bf),
            jax.ShapeDtypeStruct((8, LANES), f4),
        ],
        in_specs=[anywhere] * 4,
        out_specs=[anywhere] * 4 + [inside] * 2,
        scratch_shapes=kept,
        compiler_params=pltpu.CompilerParams(
            collective_id=0, has_side_effects=True, vmem_limit_bytes=60 * 2**20
        ),
        name="front",
    )(inputs, cotangent, weight_in, weight_out)


def row_block(rows):
    return 256 if rows % 256 == 0 else 128


def to_lanes(column_tops):
    pieces = []
    for at in range(0, column_tops.shape[0], LANES):
        turned = column_tops[at : at + LANES].T
        pieces.append(jnp.max(turned, axis=0, keepdims=True))
    return jnp.concatenate(pieces, axis=1)


def lane_fold(values, combine):
    top = values[:, :LANES]
    for at in range(LANES, values.shape[1], LANES):
        top = combine(top, values[:, at : at + LANES])
    return top


def sublane_fold(values, combine):
    top = values[:PACKED]
    for low in range(PACKED, values.shape[0], PACKED):
        top = combine(top, values[low : low + PACKED])
    return top


second_gain = ((1.0 - second_decay) / second_decay) ** 0.5
moment_gain = (1.0 - momentum_decay) / momentum_decay / second_gain
root_gain = second_decay**0.5 / momentum_decay


def moments_block(at, gain, left_ref, right_ref, sources, targets, row_ref, row_at, col_ref, turned):
    weight_ref, moment_ref, second_ref = sources
    new_moment_ref, new_second_ref = targets
    block, width = turned.shape[0], weight_ref.shape[1]
    rows = span(at * block, block)
    turned[:, :] = left_ref[:, rows].T
    tile = 256 if width % 256 == 0 else 128
    row_tops = [None, None]
    for low in range(0, width, tile):
        take = slice(low, low + tile)
        pulled = contract(turned[...], right_ref[:, take], 1, 0) * gain
        moment = moment_ref[rows, take] + (pulled * moment_gain).astype(jnp.bfloat16)
        second = second_ref[rows, take] + (pulled * pulled).astype(jnp.bfloat16)
        wide = second.astype(jnp.float32)
        root = wide * lax.rsqrt(wide)
        step = moment.astype(jnp.float32) / (root * root_gain + stable_eps / momentum_decay)
        decayed = weight_ref[rows, take] * jnp.bfloat16(weight_decay)
        weight_ref[rows, take] = step.astype(jnp.bfloat16) + decayed
        new_moment_ref[rows, take] = moment
        new_second_ref[rows, take] = second
        for which, value in enumerate((jnp.abs(moment), second)):
            top = lane_fold(value, jnp.maximum)
            row_tops[which] = top if low == 0 else jnp.maximum(row_tops[which], top)
            col_ref[which, :, take] = jnp.maximum(
                col_ref[which, :, take], sublane_fold(value, jnp.maximum)
            )
    for which in range(2):
        row_ref[row_at + which : row_at + which + 1, rows] = to_lanes(
            row_tops[which].astype(jnp.float32)
        )


def moments_kernel(
    factor_ref, inputs_hbm, delta_hbm, hidden_hbm, cotangent_hbm,
    weight_in_hbm, moment_in_hbm, second_in_hbm, weight_out_hbm, moment_out_hbm, second_out_hbm,
    update_in, update_out, new_moment_in, new_second_in, new_moment_out, new_second_out,
    by_col, by_row,
    inputs, delta, hidden, cotangent,
    weight_in, moment_in, second_in, weight_out, moment_out, second_out,
    cols_in, cols_out, turned_in, turned_out, side_sem, in_sem, out_sem, put_in, put_out,
):
    block_in, block_out = turned_in.shape[0], turned_out.shape[0]
    steps_in, steps_out = weight_in.shape[0] // block_in, weight_out.shape[0] // block_out
    sides = [
        pltpu.make_async_copy(source, target, side_sem.at[at])
        for at, (source, target) in enumerate(
            (
                (inputs_hbm, inputs), (delta_hbm, delta),
                (hidden_hbm, hidden), (cotangent_hbm, cotangent),
            )
        )
    ]
    pairs_in = (
        (weight_in_hbm, weight_in), (moment_in_hbm, moment_in), (second_in_hbm, second_in)
    )
    pairs_out = (
        (weight_out_hbm, weight_out), (moment_out_hbm, moment_out), (second_out_hbm, second_out)
    )

    def loads(pairs, sems, block, at):
        rows = span(at * block, block)
        return [
            pltpu.make_async_copy(source.at[rows, :], target.at[rows, :], sems.at[which, at])
            for which, (source, target) in enumerate(pairs)
        ]

    def begin_in(at):
        for copy in loads(pairs_in, in_sem, block_in, at):
            copy.start()

    def begin_out(at):
        for copy in loads(pairs_out, out_sem, block_out, at):
            copy.start()

    def put(source, target, sems, block, at):
        rows = span(at * block, block)
        return pltpu.make_async_copy(source.at[rows, :], target.at[rows, :], sems.at[at])

    sides[0].start()
    sides[1].start()
    for at in range(AHEAD):
        begin_in(at)
    cols_in[...] = jnp.zeros_like(cols_in)
    cols_out[...] = jnp.zeros_like(cols_out)
    gain = factor_ref[0:1, 0:1] * second_gain
    sides[0].wait()
    sides[1].wait()
    sides[2].start()
    sides[3].start()

    @pl.loop(0, steps_in)
    def _(at):
        pl.when(at + AHEAD < steps_in)(lambda: begin_in(at + AHEAD))
        pl.when(at + AHEAD >= steps_in)(lambda: begin_out(at + AHEAD - steps_in))
        for copy in loads(pairs_in, in_sem, block_in, at):
            copy.wait()
        moments_block(
            at, gain, inputs, delta, (weight_in, moment_in, second_in),
            (new_moment_in, new_second_in), by_col, 0, cols_in, turned_in,
        )
        put(weight_in, update_in, put_in, block_in, at).start()

    sides[2].wait()
    sides[3].wait()

    @pl.loop(0, steps_out)
    def _(at):
        pl.when(at + AHEAD < steps_out)(lambda: begin_out(at + AHEAD))
        for copy in loads(pairs_out, out_sem, block_out, at):
            copy.wait()
        moments_block(
            at, gain, hidden, cotangent, (weight_out, moment_out, second_out),
            (new_moment_out, new_second_out), by_row, 2, cols_out, turned_out,
        )
        put(weight_out, update_out, put_out, block_out, at).start()

    for which in range(2):
        top = cols_in[which].astype(jnp.float32)
        by_row[which : which + 1, :] = jnp.max(top, axis=0, keepdims=True)
        top = cols_out[which].astype(jnp.float32)
        by_col[which + 2 : which + 3, :] = jnp.max(top, axis=0, keepdims=True)
    for at in range(steps_in):
        put(weight_in, update_in, put_in, block_in, at).wait()
    for at in range(steps_out):
        put(weight_out, update_out, put_out, block_out, at).wait()


def held(shape):
    return pltpu.VMEM(shape, jnp.bfloat16)


def moments(factor, inputs, delta, hidden, cotangent, first, latter):
    width, units = first[0].shape
    tokens = inputs.shape[0]
    block_in, block_out = row_block(width), row_block(units)
    steps_in, steps_out = width // block_in, units // block_out
    inside = pl.BlockSpec(memory_space=pltpu.VMEM)
    anywhere = pl.BlockSpec(memory_space=pl.ANY)
    return pl.pallas_call(
        moments_kernel,
        out_shape=[
            jax.ShapeDtypeStruct((width, units), jnp.bfloat16),
            jax.ShapeDtypeStruct((units, width), jnp.bfloat16),
            held((width, units)),
            held((width, units)),
            held((units, width)),
            held((units, width)),
            pltpu.VMEM((4, width), jnp.float32),
            pltpu.VMEM((4, units), jnp.float32),
        ],
        in_specs=[inside] + [anywhere] * 10,
        out_specs=[anywhere] * 2 + [inside] * 6,
        scratch_shapes=[
            held((tokens, width)),
            held((tokens, units)),
            held((tokens, units)),
            held((tokens, width)),
        ]
        + [held((width, units))] * 3
        + [held((units, width))] * 3
        + [
            held((2, PACKED, units)),
            held((2, PACKED, width)),
            held((block_in, tokens)),
            held((block_out, tokens)),
            pltpu.SemaphoreType.DMA((4,)),
            pltpu.SemaphoreType.DMA((3, steps_in)),
            pltpu.SemaphoreType.DMA((3, steps_out)),
            pltpu.SemaphoreType.DMA((steps_in,)),
            pltpu.SemaphoreType.DMA((steps_out,)),
        ],
        compiler_params=pltpu.CompilerParams(vmem_limit_bytes=VMEM_MOMENTS),
        name="moments",
    )(factor, inputs, delta, hidden, cotangent, *first, *latter)


def tops_kernel(sizes, col_ref, row_ref, all_col, all_row, send_c, recv_c, send_r, recv_r):
    jobs = (
        ("col", col_ref, all_col, send_c, recv_c),
        ("row", row_ref, all_row, send_r, recv_r),
    )
    barrier = pltpu.get_barrier_semaphore()
    for axis, *_ in jobs:
        me = lax.axis_index(axis)
        for off in range(1, sizes[axis]):
            peer = lax.rem(me + off, sizes[axis])
            pl.semaphore_signal(barrier, inc=1, device_id={axis: peer}, device_id_type=MESH)
    pl.semaphore_wait(barrier, sizes["col"] + sizes["row"] - 2)
    copies = []
    for axis, source, target, send, receive in jobs:
        me = lax.axis_index(axis)
        for off in range(1, sizes[axis]):
            peer = lax.rem(me + off, sizes[axis])
            copy = remote(source, target.at[off], send.at[off], receive.at[off], axis, peer)
            copy.start()
            copies.append(copy)
    for _, source, target, *_ in jobs:
        target[0] = source[...]
    for copy in copies:
        copy.wait()


def exchange_tops(sizes, by_col, by_row):
    rows, cols = sizes["row"], sizes["col"]
    inside = pl.BlockSpec(memory_space=pltpu.VMEM)
    return pl.pallas_call(
        functools.partial(tops_kernel, sizes),
        out_shape=[
            pltpu.VMEM((cols,) + by_col.shape, jnp.float32),
            pltpu.VMEM((rows,) + by_row.shape, jnp.float32),
        ],
        in_specs=[inside] * 2,
        out_specs=[inside] * 2,
        scratch_shapes=[
            pltpu.SemaphoreType.DMA((cols,)),
            pltpu.SemaphoreType.DMA((cols,)),
            pltpu.SemaphoreType.DMA((rows,)),
            pltpu.SemaphoreType.DMA((rows,)),
        ],
        compiler_params=pltpu.CompilerParams(
            collective_id=1, has_side_effects=True, vmem_limit_bytes=4 * 2**20
        ),
        name="tops",
    )(*(pltpu.with_memory_space_constraint(top, pltpu.VMEM) for top in (by_col, by_row)))


def encode_block(at, block, sources, targets, row_ref, row_at, col_ref, col_at):
    cols = targets[0].shape[1]
    for which in range(2):
        source, target = sources[which], targets[which]
        for low in range(0, block, LANES):
            rows = span(at * block + low, LANES)
            inverse = row_ref[row_at + which : row_at + which + 1, rows]
            inverse = jnp.broadcast_to(inverse, (LANES, LANES)).T
            for lane in range(0, cols, LANES):
                other = col_ref[col_at + which : col_at + which + 1, lane : lane + LANES]
                value = source[rows, lane : lane + LANES].astype(jnp.float32)
                value = value * jnp.maximum(inverse, other)
                target[rows, lane : lane + LANES] = value.astype(jnp.bfloat16)


def encode_kernel(
    all_col, all_row, moment_in, second_in, moment_out, second_out, grad_from,
    code_moment_in, code_second_in, code_moment_out, code_second_out,
    row_scale_in, col_scale_in, row_scale_out, col_scale_out, grad_to,
    inverse_col, inverse_row, made_moment_in, made_second_in, made_moment_out, made_second_out,
    grad, in_sem, out_sem, grad_sem,
):
    fetch = pltpu.make_async_copy(grad_from, grad, grad_sem.at[0])
    store = pltpu.make_async_copy(grad, grad_to, grad_sem.at[1])
    fetch.start()
    for source, inverse, scales in (
        (all_col, inverse_col, (row_scale_in, col_scale_out)),
        (all_row, inverse_row, (col_scale_in, row_scale_out)),
    ):
        top = source[0]
        for at in range(1, source.shape[0]):
            top = jnp.maximum(top, source[at])
        for at in range(4):
            decay = second_decay if at % 2 else momentum_decay
            scale = jnp.maximum(top[at : at + 1] * decay, 1.0)
            scales[at // 2][at % 2 : at % 2 + 1, :] = scale
            inverse[at : at + 1, :] = decay / scale

    jobs = (
        (
            (moment_in, second_in), (made_moment_in, made_second_in),
            (code_moment_in, code_second_in), inverse_col, 0, inverse_row, 0, in_sem,
        ),
        (
            (moment_out, second_out), (made_moment_out, made_second_out),
            (code_moment_out, code_second_out), inverse_row, 2, inverse_col, 2, out_sem,
        ),
    )

    def puts(made, codes, sems, block, at):
        rows = span(at * block, block)
        return [
            pltpu.make_async_copy(made[i].at[rows, :], codes[i].at[rows, :], sems.at[i, at])
            for i in range(2)
        ]

    for sources, made, codes, row_ref, row_at, col_ref, col_at, sems in jobs:
        block = row_block(made[0].shape[0])

        @pl.loop(0, made[0].shape[0] // block)
        def _(at):
            encode_block(at, block, sources, made, row_ref, row_at, col_ref, col_at)
            for copy in puts(made, codes, sems, block, at):
                copy.start()

    fetch.wait()
    store.start()
    store.wait()
    for sources, made, codes, row_ref, row_at, col_ref, col_at, sems in jobs:
        block = row_block(made[0].shape[0])
        for at in range(made[0].shape[0] // block):
            for copy in puts(made, codes, sems, block, at):
                copy.wait()


def encode(all_col, all_row, moment_in, second_in, moment_out, second_out, input_grad):
    width, units = moment_in.shape
    inside = pl.BlockSpec(memory_space=pltpu.VMEM)
    anywhere = pl.BlockSpec(memory_space=pl.ANY)
    half, full = jnp.bfloat16, jnp.float32
    return pl.pallas_call(
        encode_kernel,
        out_shape=[
            jax.ShapeDtypeStruct((width, units), half),
            jax.ShapeDtypeStruct((width, units), half),
            jax.ShapeDtypeStruct((units, width), half),
            jax.ShapeDtypeStruct((units, width), half),
            jax.ShapeDtypeStruct((2, width), full),
            jax.ShapeDtypeStruct((2, units), full),
            jax.ShapeDtypeStruct((2, units), full),
            jax.ShapeDtypeStruct((2, width), full),
            jax.ShapeDtypeStruct(input_grad.shape, half),
        ],
        in_specs=[inside] * 6 + [anywhere],
        out_specs=[anywhere] * 4 + [inside] * 4 + [anywhere],
        scratch_shapes=[
            pltpu.VMEM((4, width), full),
            pltpu.VMEM((4, units), full),
            pltpu.VMEM((width, units), half),
            pltpu.VMEM((width, units), half),
            pltpu.VMEM((units, width), half),
            pltpu.VMEM((units, width), half),
            pltpu.VMEM(input_grad.shape, half),
            pltpu.SemaphoreType.DMA((2, width // row_block(width))),
            pltpu.SemaphoreType.DMA((2, units // row_block(units))),
            pltpu.SemaphoreType.DMA((2,)),
        ],
        compiler_params=pltpu.CompilerParams(vmem_limit_bytes=VMEM_ENCODE),
        name="encode",
    )(
        *(
            pltpu.with_memory_space_constraint(value, pltpu.VMEM)
            for value in (all_col, all_row, moment_in, second_in, moment_out, second_out)
        ),
        input_grad,
    )


def shards(
    sizes, inputs, cotangent, weight_in, moment_in, second_in, weight_out, moment_out, second_out
):
    all_inputs, all_cotangent, all_hidden, all_delta, input_grad, factor = front(
        sizes, inputs, cotangent, weight_in, weight_out
    )
    update_in, update_out, *kept, by_col, by_row = moments(
        factor,
        all_inputs,
        all_delta,
        all_hidden,
        all_cotangent,
        (weight_in, moment_in, second_in),
        (weight_out, moment_out, second_out),
    )
    all_col, all_row = exchange_tops(sizes, by_col, by_row)
    (
        code_moment_in, code_second_in, code_moment_out, code_second_out,
        rows_in, cols_in, rows_out, cols_out, input_grad,
    ) = encode(all_col, all_row, *kept, input_grad)
    return (
        input_grad,
        update_in,
        code_moment_in,
        code_second_in,
        rows_in,
        cols_in,
        update_out,
        code_moment_out,
        code_second_out,
        rows_out,
        cols_out,
    )


def solution(mesh):
    in_specs = (
        P("col", "row"),
        P("col", "row"),
        P("row", "col"),
        P("row", "col"),
        P("row", "col"),
        P("col", "row"),
        P("col", "row"),
        P("col", "row"),
    )
    out_specs = (
        P("col", "row"),
        P("row", "col"),
        P("row", "col"),
        P("row", "col"),
        P(None, "row"),
        P(None, "col"),
        P("col", "row"),
        P("col", "row"),
        P("col", "row"),
        P(None, "col"),
        P(None, "row"),
    )
    sizes = {axis: mesh.shape[axis] for axis in ("row", "col")}
    return jax.shard_map(
        functools.partial(shards, sizes),
        mesh=mesh,
        in_specs=in_specs,
        out_specs=out_specs,
        check_vma=False,
    )
```

```python
import functools

import jax
import jax.numpy as jnp
from jax import lax
from jax.experimental import pallas as pl
from jax.experimental.pallas import tpu as pltpu
from jax.sharding import PartitionSpec as P

root_half = 0.7071067811865476
normal_density = 0.3989422804014327
momentum_decay = 0.9
second_decay = 0.95
stable_eps = 1e-08
weight_decay = 0.1
LANES = 128
PACKED = 16
AHEAD = 2
VMEM_MOMENTS = 40 * 2**20
VMEM_ENCODE = 40 * 2**20


def contract(left, right, left_dim, right_dim):
    return lax.dot_general(
        left, right, (((left_dim,), (right_dim,)), ((), ())), preferred_element_type=jnp.float32
    )


def activate(preact, hidden_grad):
    cumulative = 0.5 * (1.0 + lax.erf(preact * root_half))
    density = jnp.exp(-0.5 * preact * preact) * normal_density
    hidden = (preact * cumulative).astype(jnp.bfloat16)
    delta = (hidden_grad * (cumulative + preact * density)).astype(jnp.bfloat16)
    return (hidden, delta)


MESH = pl.DeviceIdType.MESH


def remote(source, target, send, receive, axis, peer):
    return pltpu.make_async_remote_copy(
        src_ref=source,
        dst_ref=target,
        send_sem=send,
        recv_sem=receive,
        device_id={axis: peer},
        device_id_type=MESH,
    )


def span(start, size):
    return pl.ds(pl.multiple_of(start, size), size)


def lane_tile(size):
    return 512 if size % 512 == 0 else 256 if size % 256 == 0 else 128


def folded(values):
    total = values[:8, :LANES] * 0.0
    for low in range(0, values.shape[0], 8):
        for at in range(0, values.shape[1], LANES):
            total = total + values[low : low + 8, at : at + LANES]
    return total


def front_kernel(
    shape, x_ref, c_ref, wi_hbm, wo_hbm,
    x_out, c_out, hidden_out, delta_out, grad_ref, factor_ref,
    acts, wi, wo, pair_send, pair_recv, pair_own, line_send, line_recv, line_own, hd,
    dx_own, dx_send, dx_recv, dz_send, dz_recv, part_ref, col_tops, row_tops, grams,
    load_sem, z_send, z_recv, y_send, y_recv, pair_s, pair_r, line_s, line_r,
    gather_s, gather_r, share_s, share_r, dy_s, dy_r, dz_s, dz_r,
    tot_s, tot_r, row_s, row_r, out_sem,
):
    rows, cols, nx, ny, nz, entries = shape
    t, width = x_ref.shape
    hidden = wi.shape[1]
    size = ny * t
    half = t // 2
    piece = half // nx
    tokens = size * nz
    r, k = lax.axis_index("row"), lax.axis_index("col")
    x, core = r // 2, r % 2
    z, y = k // ny, k % ny
    partner = x * 2 + (1 - core)
    below, above = z, nz - 1 - z
    middle = jnp.minimum(below, above)

    def source_of(g):
        if g == 0:
            return z, 0
        near = g <= 2 * middle
        distance = jnp.where(near, (g + 1) // 2, g - middle)
        side = jnp.where(near, -1 if g % 2 else 1, jnp.where(above > below, 1, -1))
        return z + side * distance, side

    order = [source_of(g) for g in range(nz)]

    def line_peer(off):
        return lax.rem(x + off, nx) * 2 + core

    def y_peer(off):
        return z * ny + lax.rem(y + off, ny)

    loads = [
        pltpu.make_async_copy(x_ref, acts.at[0, span(k * t, t)], load_sem.at[0]),
        pltpu.make_async_copy(c_ref, acts.at[1, span(k * t, t)], load_sem.at[1]),
        pltpu.make_async_copy(wi_hbm, wi, load_sem.at[2]),
        pltpu.make_async_copy(wo_hbm, wo, load_sem.at[3]),
    ]
    for load in loads:
        load.start()
    barrier = pltpu.get_barrier_semaphore()
    for off in range(1, cols):
        pl.semaphore_signal(
            barrier, inc=1, device_id={"col": lax.rem(k + off, cols)}, device_id_type=MESH
        )
    for off in range(1, rows):
        pl.semaphore_signal(
            barrier, inc=1, device_id={"row": lax.rem(r + off, rows)}, device_id_type=MESH
        )
    loads[0].wait()
    loads[1].wait()
    pl.semaphore_wait(barrier, cols + rows - 2)

    pending = []

    def z_copy(item, zs, g, way, sign):
        block = acts.at[item, span((zs * ny + y) * t, t)]
        return remote(
            block, block, z_send.at[item, g, way], z_recv.at[item, zs], "col", (z + sign) * ny + y
        )

    def y_copies(item, zs, g):
        block = acts.at[item, span((zs * ny + y) * t, t)]
        copies = [
            remote(
                block, block, y_send.at[item, g, off], y_recv.at[item, zs, y], "col", y_peer(off)
            )
            for off in range(1, ny)
        ]
        for copy in copies:
            copy.start()
            pending.append(copy)

    ways = ((0, 1, z < nz - 1), (1, -1, z > 0))
    for item in range(2):
        for way, sign, there in ways:
            pl.when(there)(lambda i=item, w=way, s=sign: z_copy(i, z, 0, w, s).start())
        y_copies(item, z, 0)

    def onward(g):
        zs, side = order[g]
        ahead = z - side
        return zs, -side, jnp.logical_and(ahead >= 0, ahead < nz)

    def forward(g):
        zs, sign, there = onward(g)
        for item in range(2):
            block = acts.at[item, span((zs * ny + y) * t, t)]
            remote(
                block, block, z_send.at[item, g, 0], z_recv.at[item, zs], "col", y_peer(1)
            ).wait_recv()
            pl.when(there)(lambda i=item: z_copy(i, zs, g, 0, sign).start())
            y_copies(item, zs, g)

    def first_row(unit):
        g, j = unit
        return (order[g][0] * ny + lax.rem(y + j, ny)) * t

    def y_wait(g, item):
        zs, _ = order[g]
        for off in range(1, ny):
            ys = lax.rem(y + off, ny)
            block = acts.at[item, span((zs * ny + ys) * t, t)]
            remote(
                block, block, y_send.at[item, g, off], y_recv.at[item, zs, ys], "col", y_peer(1)
            ).wait_recv()

    tile_h, tile_w = lane_tile(hidden), lane_tile(width)
    chunks = width // tile_w

    def forward_product(units, item):
        left = jnp.concatenate(
            [
                acts[item, span(first_row(unit) + which * half, half), :]
                for unit in units
                for which in (1 - core, core)
            ],
            axis=0,
        )

        @pl.loop(0, hidden // tile_h)
        def _(n):
            at = span(n * tile_h, tile_h)
            if item == 0:
                part = contract(left, wi[:, at], 1, 0)
            else:
                part = contract(left, wo[at, :], 1, 1)
            for i, (g, j) in enumerate(units):
                low = i * t
                pair_send[g, j, item, :, at] = part[low : low + half]
                pair_own[g, j, item, :, at] = part[low + half : low + t]

        for unit in units:
            pair_copy(unit, item).start()
            pending.append(pair_copy(unit, item))

    def pair_copy(unit, item):
        g, j = unit
        return remote(
            pair_send.at[g, j, item], pair_recv.at[g, j, item],
            pair_s.at[item, g, j], pair_r.at[item, g, j], "row", partner,
        )

    def line_copy(unit, off):
        g, j = unit
        return remote(
            line_send.at[g, j, off - 1], line_recv.at[g, j, off - 1],
            line_s.at[g, j, off], line_r.at[g, j, off], "row", line_peer(off),
        )

    def pair_sum(unit):
        g, j = unit
        for item in range(2):
            pair_copy(unit, item).wait_recv()
        for off in range(1, nx):
            take = span(lax.rem(x + off, nx) * piece, piece)
            for item in range(2):
                line_send[g, j, off - 1, item] = (
                    pair_own[g, j, item, take, :] + pair_recv[g, j, item, take, :]
                ).astype(jnp.bfloat16)
            line_copy(unit, off).start()
            pending.append(line_copy(unit, off))
        take = span(x * piece, piece)
        for item in range(2):
            line_own[g, j, item] = pair_own[g, j, item, take, :] + pair_recv[g, j, item, take, :]

    def gather_block(unit, xs):
        return hd.at[:, span(first_row(unit) + core * half + xs * piece, piece), :]

    def gather_copy(unit, off):
        g, j = unit
        block = gather_block(unit, x)
        return remote(
            block, block, gather_s.at[g, j, off], gather_r.at[g, j, off], "row", line_peer(off)
        )

    def active(unit):
        g, j = unit
        for off in range(1, nx):
            line_copy(unit, off).wait_recv()
        first = first_row(unit) + core * half + x * piece

        @pl.loop(0, hidden // tile_h)
        def _(n):
            at = span(n * tile_h, tile_h)
            preact, hidden_grad = line_own[g, j, 0, :, at], line_own[g, j, 1, :, at]
            for off in range(1, nx):
                preact = preact + line_recv[g, j, off - 1, 0, :, at].astype(jnp.float32)
                hidden_grad = hidden_grad + line_recv[g, j, off - 1, 1, :, at].astype(jnp.float32)
            value, slope = activate(preact, hidden_grad)
            hd[0, span(first, piece), at] = value
            hd[1, span(first, piece), at] = slope

        for off in range(1, nx):
            gather_copy(unit, off).start()
            pending.append(gather_copy(unit, off))

    def share_copy(unit, which):
        block = hd.at[:, span(first_row(unit) + which * half, half), :]
        return remote(block, block, share_s.at[unit], share_r.at[unit], "row", partner)

    def share(unit):
        g, j = unit
        for off in range(1, nx):
            block = gather_block(unit, lax.rem(x + nx - off, nx))
            remote(
                block, block, gather_s.at[g, j, off], gather_r.at[g, j, off],
                "row", line_peer(off),
            ).wait_recv()
        share_copy(unit, core).start()
        pending.append(share_copy(unit, core))

    def share_wait(unit):
        share_copy(unit, 1 - core).wait_recv()

    def dx_copy(g, off, chunk):
        return remote(
            dx_send.at[g, off - 1, chunk], dx_recv.at[g, off - 1, chunk],
            dy_s.at[g, off, chunk], dy_r.at[g, off, chunk], "col", y_peer(off),
        )

    def back_product(batches):
        units = [unit for at in batches for unit in groups[at]]
        left = jnp.concatenate([hd[1, span(first_row(unit), t), :] for unit in units], axis=0)
        for chunk in range(chunks):
            part = contract(left, wi[chunk * tile_w : (chunk + 1) * tile_w, :], 1, 1)
            for i, (g, j) in enumerate(units):
                rows_of = part[i * t : (i + 1) * t]
                if j == 0:
                    dx_own[g, chunk] = rows_of
                else:
                    dx_send[g, j - 1, chunk] = rows_of.astype(jnp.bfloat16)
                    dx_copy(g, j, chunk).start()
                    pending.append(dx_copy(g, j, chunk))

    def dz_copy(g, chunk):
        return remote(
            dz_send.at[g, chunk], dz_recv.at[z, chunk], dz_s.at[g, chunk], dz_r.at[z, chunk],
            "col", order[g][0] * ny + y,
        )

    def back_sum(g):
        for chunk in range(chunks):
            total = dx_own[g, chunk]
            for off in range(1, ny):
                dx_copy(g, off, chunk).wait_recv()
                total = total + dx_recv[g, off - 1, chunk].astype(jnp.float32)
            if g == 0:
                dx_own[0, chunk] = total
            else:
                dz_send[g, chunk] = total.astype(jnp.bfloat16)
                dz_copy(g, chunk).start()
                pending.append(dz_copy(g, chunk))

    outs = []

    def put(source, target, slot):
        copy = pltpu.make_async_copy(source, target, out_sem.at[slot])
        copy.start()
        outs.append(copy)

    use_grams = grams is not None
    tile_t = 256 if tokens % 256 == 0 else 128

    def gram(which, source, item):
        @pl.loop(0, tokens // tile_t)
        def _(n):
            at = span(n * tile_t, tile_t)
            grams[which, :, at] = contract(source[item], source[item, at, :], 1, 1)

    def local_total():
        if use_grams:
            part_ref[...] = jnp.zeros_like(part_ref)

            @pl.loop(0, tokens // tile_t)
            def _(n):
                at = span(n * tile_t, tile_t)
                late_in = contract(hd[1], hd[1, at, :], 1, 1)
                part_ref[...] += folded(late_in * grams[0, :, at])
                late_out = contract(hd[0], hd[0, at, :], 1, 1)
                part_ref[...] += folded(late_out * grams[1, :, at])
        else:
            part_ref[...] = jnp.zeros_like(part_ref)
            for left, right, count in ((acts.at[0], hd.at[1], width), (hd.at[0], acts.at[1], hidden)):

                @pl.loop(0, count // LANES)
                def _(n):
                    at = span(n * LANES, LANES)
                    part = contract(left[:, at], right[...], 0, 0)
                    part_ref[...] += folded(part * part)

    others = range(1, ny)
    groups = [[(0, 0)]]
    groups += [[(g - 1, j) for j in others] + [(g, 0)] for g in range(1, nz)]
    groups += [[(nz - 1, j) for j in others]]

    for s in range(nz + 4):
        if 1 <= s < nz:
            forward(s)
        if s <= nz:
            for item in range(2):
                if s >= 1:
                    y_wait(s - 1, item)
                else:
                    loads[2 + item].wait()
                forward_product(groups[s], item)
        if s == nz:
            put(acts.at[0], x_out, 0)
            put(acts.at[1], c_out, 1)
        if 0 <= s - 1 <= nz:
            for unit in groups[s - 1]:
                active(unit)
        if s <= nz:
            for unit in groups[s]:
                pair_sum(unit)
        if 0 <= s - 2 <= nz:
            for unit in groups[s - 2]:
                share(unit)
        if 0 <= s - 3 <= nz:
            for unit in groups[s - 3]:
                share_wait(unit)
        if s == nz:
            back_product(list(range(nz - 2)))
            if use_grams:
                gram(0, acts, 0)
                gram(1, acts, 1)
        if s == nz + 1:
            back_product([nz - 2])
            for g in range(nz - 3):
                back_sum(g)
        if s == nz + 2:
            back_product([nz - 1])
            back_sum(nz - 3)
    put(hd.at[0], hidden_out, 2)
    put(hd.at[1], delta_out, 3)
    back_product([nz])
    back_sum(nz - 2)
    local_total()

    def col_copy(off):
        return remote(
            part_ref, col_tops.at[off], tot_s.at[off], tot_r.at[off],
            "col", lax.rem(k + off, cols),
        )

    def row_copy(off):
        return remote(
            col_tops.at[0], row_tops.at[off], row_s.at[off], row_r.at[off],
            "row", lax.rem(r + off, rows),
        )

    for off in range(1, cols):
        col_copy(off).start()
        pending.append(col_copy(off))
    back_sum(nz - 1)
    for off in range(1, cols):
        col_copy(off).wait_recv()
    total = part_ref[...]
    for off in range(1, cols):
        total = total + col_tops[off]
    col_tops[0] = total
    for off in range(1, rows):
        row_copy(off).start()
        pending.append(row_copy(off))
    for off in range(1, rows):
        row_copy(off).wait_recv()
        total = total + row_tops[off]
    total = jnp.sum(jnp.sum(total, axis=0, keepdims=True), axis=1, keepdims=True)
    total = jnp.maximum(total, 0.0)
    factor = 1.0 / jnp.maximum(jnp.sqrt(total / entries), 1.0)
    factor_ref[...] = jnp.broadcast_to(factor, factor_ref.shape)

    for chunk in range(chunks):
        total = dx_own[0, chunk]
        for off in range(1, nz):
            zs = lax.rem(z + off, nz)
            remote(
                dz_send.at[1, chunk], dz_recv.at[zs, chunk],
                dz_s.at[1, chunk], dz_r.at[zs, chunk], "col", y_peer(1),
            ).wait_recv()
            total = total + dz_recv[zs, chunk].astype(jnp.float32)
        grad_ref[:, chunk * tile_w : (chunk + 1) * tile_w] = total.astype(jnp.bfloat16)

    for item in range(2):
        for way, sign, there in ways:
            pl.when(there)(lambda i=item, w=way, s=sign: z_copy(i, z, 0, w, s).wait_send())
    for g in range(1, nz):
        zs, sign, there = onward(g)
        for item in range(2):
            pl.when(there)(lambda i=item, a=zs, b=g, s=sign: z_copy(i, a, b, 0, s).wait_send())
    for copy in pending:
        copy.wait_send()
    for copy in outs:
        copy.wait()


def front(sizes, inputs, cotangent, weight_in, weight_out):
    rows, cols = sizes["row"], sizes["col"]
    nx = rows // 2
    ny = 2 ** ((cols.bit_length() - 1) // 2)
    nz = cols // ny
    t, width = inputs.shape
    hidden = weight_in.shape[1]
    size = t * ny
    half, tokens = t // 2, size * nz
    piece = half // nx
    tile = lane_tile(width)
    parts = (width // tile, t, tile)
    entries = 2.0 * width * rows * hidden * cols
    bf, f4 = jnp.bfloat16, jnp.float32
    use_grams = tokens <= hidden
    dma = lambda *dims: pltpu.SemaphoreType.DMA(dims)
    scratch = [
        pltpu.VMEM((2, tokens, width), bf),
        pltpu.VMEM(weight_in.shape, bf),
        pltpu.VMEM(weight_out.shape, bf),
        pltpu.VMEM((nz, ny, 2, half, hidden), f4),
        pltpu.VMEM((nz, ny, 2, half, hidden), f4),
        pltpu.VMEM((nz, ny, 2, half, hidden), f4),
        pltpu.VMEM((nz, ny, nx - 1, 2, piece, hidden), bf),
        pltpu.VMEM((nz, ny, nx - 1, 2, piece, hidden), bf),
        pltpu.VMEM((nz, ny, 2, piece, hidden), f4),
        pltpu.VMEM((2, tokens, hidden), bf),
        pltpu.VMEM((nz,) + parts, f4),
        pltpu.VMEM((nz, ny - 1) + parts, bf),
        pltpu.VMEM((nz, ny - 1) + parts, bf),
        pltpu.VMEM((nz,) + parts, bf),
        pltpu.VMEM((nz,) + parts, bf),
        pltpu.VMEM((8, LANES), f4),
        pltpu.VMEM((cols, 8, LANES), f4),
        pltpu.VMEM((rows, 8, LANES), f4),
        pltpu.VMEM((2, tokens, tokens), f4) if use_grams else None,
        dma(4),
        dma(2, nz, 2), dma(2, nz), dma(2, nz, ny), dma(2, nz, ny),
        dma(2, nz, ny), dma(2, nz, ny), dma(nz, ny, nx), dma(nz, ny, nx),
        dma(nz, ny, nx), dma(nz, ny, nx), dma(nz, ny), dma(nz, ny),
        dma(nz, ny, parts[0]), dma(nz, ny, parts[0]), dma(nz, parts[0]), dma(nz, parts[0]),
        dma(cols), dma(cols), dma(rows), dma(rows), dma(4),
    ]
    kept = [item for item in scratch if item is not None]
    slot = 10 + scratch.index(None) if None in scratch else None

    def kernel(*refs):
        refs = list(refs)
        if slot is not None:
            refs.insert(slot, None)
        front_kernel((rows, cols, nx, ny, nz, entries), *refs)

    anywhere = pl.BlockSpec(memory_space=pl.ANY)
    inside = pl.BlockSpec(memory_space=pltpu.VMEM)
    return pl.pallas_call(
        kernel,
        out_shape=[
            jax.ShapeDtypeStruct((tokens, width), bf),
            jax.ShapeDtypeStruct((tokens, width), bf),
            jax.ShapeDtypeStruct((tokens, hidden), bf),
            jax.ShapeDtypeStruct((tokens, hidden), bf),
            jax.ShapeDtypeStruct((t, width), bf),
            jax.ShapeDtypeStruct((8, LANES), f4),
        ],
        in_specs=[anywhere] * 4,
        out_specs=[anywhere] * 4 + [inside] * 2,
        scratch_shapes=kept,
        compiler_params=pltpu.CompilerParams(
            collective_id=0, has_side_effects=True, vmem_limit_bytes=60 * 2**20
        ),
        name="front",
    )(inputs, cotangent, weight_in, weight_out)


def row_block(rows):
    return 256 if rows % 256 == 0 else 128


def to_lanes(column_tops):
    pieces = []
    for at in range(0, column_tops.shape[0], LANES):
        turned = column_tops[at : at + LANES].T
        pieces.append(jnp.max(turned, axis=0, keepdims=True))
    return jnp.concatenate(pieces, axis=1)


def lane_fold(values, combine):
    top = values[:, :LANES]
    for at in range(LANES, values.shape[1], LANES):
        top = combine(top, values[:, at : at + LANES])
    return top


def sublane_fold(values, combine):
    top = values[:PACKED]
    for low in range(PACKED, values.shape[0], PACKED):
        top = combine(top, values[low : low + PACKED])
    return top


second_gain = ((1.0 - second_decay) / second_decay) ** 0.5
moment_gain = (1.0 - momentum_decay) / momentum_decay / second_gain
root_gain = second_decay**0.5 / momentum_decay


def moments_block(at, gain, left_ref, right_ref, sources, targets, row_ref, row_at, col_ref, turned):
    weight_ref, moment_ref, second_ref = sources
    new_moment_ref, new_second_ref = targets
    block, width = turned.shape[0], weight_ref.shape[1]
    rows = span(at * block, block)
    turned[:, :] = left_ref[:, rows].T
    tile = 256 if width % 256 == 0 else 128
    row_tops = [None, None]
    for low in range(0, width, tile):
        take = slice(low, low + tile)
        pulled = contract(turned[...], right_ref[:, take], 1, 0) * gain
        moment = moment_ref[rows, take] + (pulled * moment_gain).astype(jnp.bfloat16)
        second = second_ref[rows, take] + (pulled * pulled).astype(jnp.bfloat16)
        wide = second.astype(jnp.float32)
        root = wide * lax.rsqrt(wide)
        step = moment.astype(jnp.float32) / (root * root_gain + stable_eps / momentum_decay)
        decayed = weight_ref[rows, take] * jnp.bfloat16(weight_decay)
        weight_ref[rows, take] = step.astype(jnp.bfloat16) + decayed
        new_moment_ref[rows, take] = moment
        new_second_ref[rows, take] = second
        for which, value in enumerate((jnp.abs(moment), second)):
            top = lane_fold(value, jnp.maximum)
            row_tops[which] = top if low == 0 else jnp.maximum(row_tops[which], top)
            col_ref[which, :, take] = jnp.maximum(
                col_ref[which, :, take], sublane_fold(value, jnp.maximum)
            )
    for which in range(2):
        row_ref[row_at + which : row_at + which + 1, rows] = to_lanes(
            row_tops[which].astype(jnp.float32)
        )


def moments_kernel(
    factor_ref, inputs_hbm, delta_hbm, hidden_hbm, cotangent_hbm,
    weight_in_hbm, moment_in_hbm, second_in_hbm, weight_out_hbm, moment_out_hbm, second_out_hbm,
    update_in, update_out, new_moment_in, new_second_in, new_moment_out, new_second_out,
    by_col, by_row,
    inputs, delta, hidden, cotangent,
    weight_in, moment_in, second_in, weight_out, moment_out, second_out,
    cols_in, cols_out, turned_in, turned_out, side_sem, in_sem, out_sem, put_in, put_out,
):
    block_in, block_out = turned_in.shape[0], turned_out.shape[0]
    steps_in, steps_out = weight_in.shape[0] // block_in, weight_out.shape[0] // block_out
    sides = [
        pltpu.make_async_copy(source, target, side_sem.at[at])
        for at, (source, target) in enumerate(
            (
                (inputs_hbm, inputs), (delta_hbm, delta),
                (hidden_hbm, hidden), (cotangent_hbm, cotangent),
            )
        )
    ]
    pairs_in = (
        (weight_in_hbm, weight_in), (moment_in_hbm, moment_in), (second_in_hbm, second_in)
    )
    pairs_out = (
        (weight_out_hbm, weight_out), (moment_out_hbm, moment_out), (second_out_hbm, second_out)
    )

    def loads(pairs, sems, block, at):
        rows = span(at * block, block)
        return [
            pltpu.make_async_copy(source.at[rows, :], target.at[rows, :], sems.at[which, at])
            for which, (source, target) in enumerate(pairs)
        ]

    def begin_in(at):
        for copy in loads(pairs_in, in_sem, block_in, at):
            copy.start()

    def begin_out(at):
        for copy in loads(pairs_out, out_sem, block_out, at):
            copy.start()

    def put(source, target, sems, block, at):
        rows = span(at * block, block)
        return pltpu.make_async_copy(source.at[rows, :], target.at[rows, :], sems.at[at])

    sides[0].start()
    sides[1].start()
    begin_in(0)
    cols_in[...] = jnp.zeros_like(cols_in)
    cols_out[...] = jnp.zeros_like(cols_out)
    gain = factor_ref[0:1, 0:1] * second_gain
    sides[0].wait()
    sides[1].wait()
    for at in range(1, AHEAD):
        begin_in(at)

    @pl.loop(0, steps_in)
    def _(at):
        pl.when(at == min(1, steps_in - 1))(sides[2].start)
        pl.when(at == min(2, steps_in - 1))(sides[3].start)
        pl.when(at + AHEAD < steps_in)(lambda: begin_in(at + AHEAD))
        pl.when(at + AHEAD >= steps_in)(lambda: begin_out(at + AHEAD - steps_in))
        for copy in loads(pairs_in, in_sem, block_in, at):
            copy.wait()
        moments_block(
            at, gain, inputs, delta, (weight_in, moment_in, second_in),
            (new_moment_in, new_second_in), by_col, 0, cols_in, turned_in,
        )
        put(weight_in, update_in, put_in, block_in, at).start()

    sides[2].wait()
    sides[3].wait()

    @pl.loop(0, steps_out)
    def _(at):
        pl.when(at + AHEAD < steps_out)(lambda: begin_out(at + AHEAD))
        for copy in loads(pairs_out, out_sem, block_out, at):
            copy.wait()
        moments_block(
            at, gain, hidden, cotangent, (weight_out, moment_out, second_out),
            (new_moment_out, new_second_out), by_row, 2, cols_out, turned_out,
        )
        put(weight_out, update_out, put_out, block_out, at).start()

    for which in range(2):
        top = cols_in[which].astype(jnp.float32)
        by_row[which : which + 1, :] = jnp.max(top, axis=0, keepdims=True)
        top = cols_out[which].astype(jnp.float32)
        by_col[which + 2 : which + 3, :] = jnp.max(top, axis=0, keepdims=True)
    for at in range(steps_in):
        put(weight_in, update_in, put_in, block_in, at).wait()
    for at in range(steps_out):
        put(weight_out, update_out, put_out, block_out, at).wait()


def held(shape):
    return pltpu.VMEM(shape, jnp.bfloat16)


def moments(factor, inputs, delta, hidden, cotangent, first, latter):
    width, units = first[0].shape
    tokens = inputs.shape[0]
    block_in, block_out = row_block(width), row_block(units)
    steps_in, steps_out = width // block_in, units // block_out
    inside = pl.BlockSpec(memory_space=pltpu.VMEM)
    anywhere = pl.BlockSpec(memory_space=pl.ANY)
    return pl.pallas_call(
        moments_kernel,
        out_shape=[
            jax.ShapeDtypeStruct((width, units), jnp.bfloat16),
            jax.ShapeDtypeStruct((units, width), jnp.bfloat16),
            held((width, units)),
            held((width, units)),
            held((units, width)),
            held((units, width)),
            pltpu.VMEM((4, width), jnp.float32),
            pltpu.VMEM((4, units), jnp.float32),
        ],
        in_specs=[inside] + [anywhere] * 10,
        out_specs=[anywhere] * 2 + [inside] * 6,
        scratch_shapes=[
            held((tokens, width)),
            held((tokens, units)),
            held((tokens, units)),
            held((tokens, width)),
        ]
        + [held((width, units))] * 3
        + [held((units, width))] * 3
        + [
            held((2, PACKED, units)),
            held((2, PACKED, width)),
            held((block_in, tokens)),
            held((block_out, tokens)),
            pltpu.SemaphoreType.DMA((4,)),
            pltpu.SemaphoreType.DMA((3, steps_in)),
            pltpu.SemaphoreType.DMA((3, steps_out)),
            pltpu.SemaphoreType.DMA((steps_in,)),
            pltpu.SemaphoreType.DMA((steps_out,)),
        ],
        compiler_params=pltpu.CompilerParams(vmem_limit_bytes=VMEM_MOMENTS),
        name="moments",
    )(factor, inputs, delta, hidden, cotangent, *first, *latter)


def tops_kernel(sizes, col_ref, row_ref, all_col, all_row, send_c, recv_c, send_r, recv_r):
    jobs = (
        ("col", col_ref, all_col, send_c, recv_c),
        ("row", row_ref, all_row, send_r, recv_r),
    )
    barrier = pltpu.get_barrier_semaphore()
    for axis, *_ in jobs:
        me = lax.axis_index(axis)
        for off in range(1, sizes[axis]):
            peer = lax.rem(me + off, sizes[axis])
            pl.semaphore_signal(barrier, inc=1, device_id={axis: peer}, device_id_type=MESH)
    pl.semaphore_wait(barrier, sizes["col"] + sizes["row"] - 2)
    copies = []
    for axis, source, target, send, receive in jobs:
        me = lax.axis_index(axis)
        for off in range(1, sizes[axis]):
            peer = lax.rem(me + off, sizes[axis])
            copy = remote(source, target.at[off], send.at[off], receive.at[off], axis, peer)
            copy.start()
            copies.append(copy)
    for _, source, target, *_ in jobs:
        target[0] = source[...]
    for copy in copies:
        copy.wait()


def exchange_tops(sizes, by_col, by_row):
    rows, cols = sizes["row"], sizes["col"]
    inside = pl.BlockSpec(memory_space=pltpu.VMEM)
    return pl.pallas_call(
        functools.partial(tops_kernel, sizes),
        out_shape=[
            pltpu.VMEM((cols,) + by_col.shape, jnp.float32),
            pltpu.VMEM((rows,) + by_row.shape, jnp.float32),
        ],
        in_specs=[inside] * 2,
        out_specs=[inside] * 2,
        scratch_shapes=[
            pltpu.SemaphoreType.DMA((cols,)),
            pltpu.SemaphoreType.DMA((cols,)),
            pltpu.SemaphoreType.DMA((rows,)),
            pltpu.SemaphoreType.DMA((rows,)),
        ],
        compiler_params=pltpu.CompilerParams(
            collective_id=1, has_side_effects=True, vmem_limit_bytes=4 * 2**20
        ),
        name="tops",
    )(*(pltpu.with_memory_space_constraint(top, pltpu.VMEM) for top in (by_col, by_row)))


def encode_block(at, block, sources, targets, row_ref, row_at, col_ref, col_at):
    cols = targets[0].shape[1]
    for which in range(2):
        source, target = sources[which], targets[which]
        for low in range(0, block, LANES):
            rows = span(at * block + low, LANES)
            inverse = row_ref[row_at + which : row_at + which + 1, rows]
            inverse = jnp.broadcast_to(inverse, (LANES, LANES)).T
            for lane in range(0, cols, LANES):
                other = col_ref[col_at + which : col_at + which + 1, lane : lane + LANES]
                value = source[rows, lane : lane + LANES].astype(jnp.float32)
                value = value * jnp.maximum(inverse, other)
                target[rows, lane : lane + LANES] = value.astype(jnp.bfloat16)


def encode_kernel(
    all_col, all_row, moment_in, second_in, moment_out, second_out, grad_from,
    code_moment_in, code_second_in, code_moment_out, code_second_out,
    row_scale_in, col_scale_in, row_scale_out, col_scale_out, grad_to,
    inverse_col, inverse_row, made_moment_in, made_second_in, made_moment_out, made_second_out,
    grad, in_sem, out_sem, grad_sem,
):
    fetch = pltpu.make_async_copy(grad_from, grad, grad_sem.at[0])
    store = pltpu.make_async_copy(grad, grad_to, grad_sem.at[1])
    fetch.start()
    for source, inverse, scales in (
        (all_col, inverse_col, (row_scale_in, col_scale_out)),
        (all_row, inverse_row, (col_scale_in, row_scale_out)),
    ):
        top = source[0]
        for at in range(1, source.shape[0]):
            top = jnp.maximum(top, source[at])
        for at in range(4):
            decay = second_decay if at % 2 else momentum_decay
            scale = jnp.maximum(top[at : at + 1] * decay, 1.0)
            scales[at // 2][at % 2 : at % 2 + 1, :] = scale
            inverse[at : at + 1, :] = decay / scale

    jobs = (
        (
            (moment_in, second_in), (made_moment_in, made_second_in),
            (code_moment_in, code_second_in), inverse_col, 0, inverse_row, 0, in_sem,
        ),
        (
            (moment_out, second_out), (made_moment_out, made_second_out),
            (code_moment_out, code_second_out), inverse_row, 2, inverse_col, 2, out_sem,
        ),
    )

    def puts(made, codes, sems, block, at):
        rows = span(at * block, block)
        return [
            pltpu.make_async_copy(made[i].at[rows, :], codes[i].at[rows, :], sems.at[i, at])
            for i in range(2)
        ]

    for sources, made, codes, row_ref, row_at, col_ref, col_at, sems in jobs:
        block = row_block(made[0].shape[0])

        @pl.loop(0, made[0].shape[0] // block)
        def _(at):
            encode_block(at, block, sources, made, row_ref, row_at, col_ref, col_at)
            for copy in puts(made, codes, sems, block, at):
                copy.start()

    fetch.wait()
    store.start()
    store.wait()
    for sources, made, codes, row_ref, row_at, col_ref, col_at, sems in jobs:
        block = row_block(made[0].shape[0])
        for at in range(made[0].shape[0] // block):
            for copy in puts(made, codes, sems, block, at):
                copy.wait()


def encode(all_col, all_row, moment_in, second_in, moment_out, second_out, input_grad):
    width, units = moment_in.shape
    inside = pl.BlockSpec(memory_space=pltpu.VMEM)
    anywhere = pl.BlockSpec(memory_space=pl.ANY)
    half, full = jnp.bfloat16, jnp.float32
    return pl.pallas_call(
        encode_kernel,
        out_shape=[
            jax.ShapeDtypeStruct((width, units), half),
            jax.ShapeDtypeStruct((width, units), half),
            jax.ShapeDtypeStruct((units, width), half),
            jax.ShapeDtypeStruct((units, width), half),
            jax.ShapeDtypeStruct((2, width), full),
            jax.ShapeDtypeStruct((2, units), full),
            jax.ShapeDtypeStruct((2, units), full),
            jax.ShapeDtypeStruct((2, width), full),
            jax.ShapeDtypeStruct(input_grad.shape, half),
        ],
        in_specs=[inside] * 6 + [anywhere],
        out_specs=[anywhere] * 4 + [inside] * 4 + [anywhere],
        scratch_shapes=[
            pltpu.VMEM((4, width), full),
            pltpu.VMEM((4, units), full),
            pltpu.VMEM((width, units), half),
            pltpu.VMEM((width, units), half),
            pltpu.VMEM((units, width), half),
            pltpu.VMEM((units, width), half),
            pltpu.VMEM(input_grad.shape, half),
            pltpu.SemaphoreType.DMA((2, width // row_block(width))),
            pltpu.SemaphoreType.DMA((2, units // row_block(units))),
            pltpu.SemaphoreType.DMA((2,)),
        ],
        compiler_params=pltpu.CompilerParams(vmem_limit_bytes=VMEM_ENCODE),
        name="encode",
    )(
        *(
            pltpu.with_memory_space_constraint(value, pltpu.VMEM)
            for value in (all_col, all_row, moment_in, second_in, moment_out, second_out)
        ),
        input_grad,
    )


def shards(
    sizes, inputs, cotangent, weight_in, moment_in, second_in, weight_out, moment_out, second_out
):
    all_inputs, all_cotangent, all_hidden, all_delta, input_grad, factor = front(
        sizes, inputs, cotangent, weight_in, weight_out
    )
    update_in, update_out, *kept, by_col, by_row = moments(
        factor,
        all_inputs,
        all_delta,
        all_hidden,
        all_cotangent,
        (weight_in, moment_in, second_in),
        (weight_out, moment_out, second_out),
    )
    all_col, all_row = exchange_tops(sizes, by_col, by_row)
    (
        code_moment_in, code_second_in, code_moment_out, code_second_out,
        rows_in, cols_in, rows_out, cols_out, input_grad,
    ) = encode(all_col, all_row, *kept, input_grad)
    return (
        input_grad,
        update_in,
        code_moment_in,
        code_second_in,
        rows_in,
        cols_in,
        update_out,
        code_moment_out,
        code_second_out,
        rows_out,
        cols_out,
    )


def solution(mesh):
    in_specs = (
        P("col", "row"),
        P("col", "row"),
        P("row", "col"),
        P("row", "col"),
        P("row", "col"),
        P("col", "row"),
        P("col", "row"),
        P("col", "row"),
    )
    out_specs = (
        P("col", "row"),
        P("row", "col"),
        P("row", "col"),
        P("row", "col"),
        P(None, "row"),
        P(None, "col"),
        P("col", "row"),
        P("col", "row"),
        P("col", "row"),
        P(None, "col"),
        P(None, "row"),
    )
    sizes = {axis: mesh.shape[axis] for axis in ("row", "col")}
    return jax.shard_map(
        functools.partial(shards, sizes),
        mesh=mesh,
        in_specs=in_specs,
        out_specs=out_specs,
        check_vma=False,
    )
```
